32 devices in a mesh: vocab: 16 (over z, y, x), dp: 2 (over core).
Axes of the slice: x: 2, y: 2, z: 4, core: 2. Of those that a mesh axis runs over, the one named last changes fastest.
Arguments:
- embed_table: bfloat16 [16384, 4096], P('vocab'), may hold values from -3 to 3
- token_ids: int32 [2, 16384], P('dp', 'vocab'), may hold values from 0 to 16383, as said below
- grad_rows: bfloat16 [2, 16384, 4096], P('dp', 'vocab'), may hold values from -12 to 12
Outputs:
- updated: bfloat16 [16384, 4096], P('vocab', 'dp')
- grad_rms: float32 [1], replicated
The draws below stay inside these ranges and needn't reach their ends.
Inputs may be any that keep to these rules, and one draw needn't show every extreme that they name: `token_ids`: rows are read cyclically: row r stands for every r + k * 16384. The window of vocab index v (tokens v * 1024 to (v + 1) * 1024 - 1 of a replica) holds ids that, read as the cyclic representatives from v * 1024 - 256 to (v + 1) * 1024 + 255, rise (never fall) along its tokens; both ends are reached in some window. Only its first 128 and last 128 tokens may lie outside rows v * 1024 to (v + 1) * 1024 - 1 (so read), the first ones below, the last ones above; in every window its first token lies below and its last above, in some window all first 128 lie below, in some all last 128 above.
All inputs are finite; a program needn't handle non-finite values.
Results may differ from the reference program's by a relative error of at most 0.002.
Values may be sent and summed in bfloat16 or wider, within the bound.
A program may use at most 128 MiB of HBM per device.

```python
import jax
import jax.numpy as jnp

D = 4096
ROWS_DEV = 1024
EDGE = 256
TOK_EDGE = 128
TOK_DEV = 1024
VOCAB = 16384
TOKENS = 16384
N_DP = 2


def draw_replica(key):
    windows = TOKENS // TOK_DEV
    key_above, key_below, key_first, key_middle, key_last = jax.random.split(key, 5)
    below = jax.random.randint(key_below, (windows,), 1, EDGE + 1)
    below = below.at[1].set(EDGE)
    above = jax.random.randint(key_above, (windows,), 1, EDGE + 1)
    above = above.at[windows - 1].set(EDGE)
    reach_up = jnp.roll(above, -1)
    device_ids = jnp.arange(windows, dtype=jnp.int32)
    starts = device_ids * ROWS_DEV
    first_low = starts - below
    first_high = jnp.where(device_ids == 1, starts, starts + ROWS_DEV // 2)
    last_low = jnp.where(device_ids == windows - 2, starts + ROWS_DEV, starts + ROWS_DEV - ROWS_DEV // 2)
    last_high = starts + ROWS_DEV + reach_up
    first_group = jax.random.randint(key_first, (windows, TOK_EDGE), first_low[:, None], first_high[:, None])
    first_group = first_group.at[:, 0].set(first_low)
    middle_group = jax.random.randint(key_middle, (windows, TOK_DEV - 2 * TOK_EDGE), starts[:, None], starts[:, None] + ROWS_DEV)
    last_group = jax.random.randint(key_last, (windows, TOK_EDGE), last_low[:, None], last_high[:, None])
    last_group = last_group.at[:, TOK_EDGE - 1].set(last_high - 1)
    window_ids = jnp.sort(jnp.concatenate([first_group, middle_group, last_group], axis=1), axis=1)
    window_ids = jnp.mod(window_ids, windows * ROWS_DEV)
    return window_ids.reshape(windows * TOK_DEV).astype(jnp.int32)


def draw_token_ids(key, part):
    replica_keys = jax.random.split(jax.random.fold_in(key, 11), N_DP)
    return jnp.stack([draw_replica(replica_keys[index]) for index in range(N_DP)])


def draw_grad_rows(key, part):
    windows = TOKENS // TOK_DEV
    key_base = jax.random.fold_in(jax.random.fold_in(key, 23), 0)
    key_window = jax.random.fold_in(jax.random.fold_in(key, 23), 3)
    values = jax.random.normal(key_base, (N_DP, TOKENS, D), jnp.float32)
    window_scale = jnp.exp(jax.random.uniform(key_window, (N_DP, windows, 1), jnp.float32, -1.2, 1.2))
    window_scale = jnp.repeat(window_scale, TOK_DEV, axis=1)
    values = window_scale * values
    return jnp.clip(values, -12.0, 12.0).astype(jnp.bfloat16)


def block_levels(own_key, extent, shards, least, high):
    gain = 1.0
    for axis_at, blocks in shards:
        steps = jax.random.uniform(jax.random.fold_in(jax.random.fold_in(own_key, 6), axis_at), (blocks,), jnp.float32, least / len(shards), high / len(shards))
        gain = gain * jnp.repeat(jnp.exp(steps), extent[axis_at] // blocks).reshape((-1,) + (1,) * (len(extent) - 1 - axis_at))
    return gain


def centred(own_key, shape, width, limit, cuts=(), kind=jnp.bfloat16):
    entries = width * jax.random.normal(own_key, shape, jnp.float32)
    if cuts:
        entries = entries * block_levels(own_key, shape, cuts, -0.22, 0.18)
    return jnp.clip(entries, -limit, limit).astype(kind)


def setup_inputs(seed: int = 0) -> dict:
    streams_of = jax.random.split(jax.random.key(seed), 4)
    embed_table = centred(streams_of[0], (VOCAB, D), 0.5, 3.0, ((0, 16),))
    token_ids = draw_token_ids(jax.random.fold_in(streams_of[3], 71), 0)
    grad_rows = draw_grad_rows(jax.random.fold_in(streams_of[3], 71), 0)
    return {"embed_table": embed_table, "token_ids": token_ids, "grad_rows": grad_rows}


step_rate = 0.5
norm_limit = 1.0

def reference(embed_table, token_ids, grad_rows):
    gradient = jnp.zeros((VOCAB, D), jnp.float32)
    for replica in range(N_DP):
        gradient = gradient + jax.ops.segment_sum(grad_rows[replica].astype(jnp.float32), token_ids[replica], num_segments=VOCAB)
    grad_rms = jnp.sqrt(jnp.sum(gradient * gradient) / (VOCAB * D))
    clip_scale = 1.0 / jnp.maximum(1.0, grad_rms / norm_limit)
    updated = (embed_table.astype(jnp.float32) - step_rate * clip_scale * gradient).astype(jnp.bfloat16)
    return (updated, jnp.reshape(grad_rms, (1,)))
```

```python
import functools

import jax
import jax.numpy as jnp
from jax import lax
from jax.experimental import pallas as pl
from jax.experimental.pallas import tpu as pltpu
from jax.sharding import PartitionSpec as P

MESH = pl.DeviceIdType.MESH
TOK_EDGE = 128
EDGE = 256
COLS = 512
STORE_ROWS = 32

step_rate = 0.5
norm_limit = 1.0


def chunk_plan(half):
    quarter = half // 4
    narrow = 128
    return (
        (0, 0, quarter),
        (1, 0, 2 * quarter),
        (1, 2 * quarter, 2 * quarter),
        (0, quarter, quarter),
        (0, 2 * quarter, quarter),
        (0, 3 * quarter, quarter - narrow),
        (0, half - narrow, narrow),
    )


def kernel(sizes, table_ref, ids_ref, grad_ref, grad, table, norm_ref,
           toks, halo, stage, own_ids, mate_ids, halo_ids, square, sums,
           own_sem, own_id_sem, table_sem, stage_sem, mate_sem, mate_id_sem,
           halo_send, halo_recv, halo_id_send, halo_id_recv, sum_send, sum_recv, known_sem):
    n_vocab, n_dp = sizes
    rows, width = table_ref.shape
    tokens = ids_ref.shape[1]
    half = width // n_dp
    n = n_vocab * n_dp
    blocks = rows // EDGE
    bits = n_vocab.bit_length() - 1
    plan = chunk_plan(half)
    v = lax.axis_index("vocab")
    p = lax.axis_index("dp")
    me = v * n_dp + p
    mate = 1 - p
    odd = lax.rem(v, 2)
    below = lax.rem(v + n_vocab - 1, n_vocab)
    above = lax.rem(v + 1, n_vocab)
    steps = [(1 << k) - 2 * (1 << k) * lax.rem(v // (1 << k), 2) for k in range(bits)]

    def across(mask):
        return functools.reduce(lambda a, b: a + b, [steps[k] for k in range(bits) if mask >> k & 1], v)

    partner = across(1)
    far = jnp.where(odd == 1, above, below)
    last = tokens - TOK_EDGE
    targets = (partner, far)
    firsts = tuple(
        pl.multiple_of(first, TOK_EDGE) for first in ((1 - odd) * last, odd * last)
    )
    bases = tuple(
        pl.multiple_of(base, EDGE) for base in ((1 - odd) * (rows - EDGE), odd * (rows - EDGE))
    )

    def columns(core, start, count):
        return pl.ds(pl.multiple_of(core * half + start, 128), count)

    def remote(src, dst, send, recv, device):
        return pltpu.make_async_remote_copy(
            src_ref=src, dst_ref=dst, send_sem=send, recv_sem=recv,
            device_id={"vocab": device[0], "dp": device[1]}, device_id_type=MESH,
        )

    stage_copies = [
        pltpu.make_async_copy(
            grad_ref.at[0, pl.ds(firsts[0], TOK_EDGE), pl.ds(core * half, plan[0][2])],
            stage.at[core], stage_sem.at[core],
        )
        for core in range(n_dp)
    ]
    for copy in stage_copies:
        copy.start()
    barrier = pltpu.get_barrier_semaphore()
    greeted = [(partner, core) for core in range(n_dp)] + [(v, mate)]
    greeted += [(across(1 << k), p) for k in range(1, bits)]
    for w, core in greeted:
        pl.semaphore_signal(
            barrier, inc=1, device_id={"vocab": w, "dp": core}, device_id_type=MESH
        )
    own_half = pl.ds(pl.multiple_of(p * half, half), half)
    own_copy = pltpu.make_async_copy(
        grad_ref.at[0, :, own_half], toks.at[pl.ds(0, tokens), :], own_sem
    )
    own_copy.start()
    own_id_copy = pltpu.make_async_copy(ids_ref, own_ids, own_id_sem)
    own_id_copy.start()
    table_copy = pltpu.make_async_copy(table_ref.at[:, own_half], table, table_sem)
    for copy in stage_copies:
        copy.wait()
    pl.semaphore_wait(barrier, len(greeted))

    def send_chunk(at):
        k, start, count = plan[at]
        for core in range(n_dp):
            src = stage.at[core] if at == 0 else grad_ref.at[
                0, pl.ds(firsts[k], TOK_EDGE), pl.ds(core * half + start, count)
            ]
            remote(
                src, halo.at[k, p, :, pl.ds(start, count)],
                halo_send, halo_recv.at[at], (targets[k], core),
            ).start()

    def send_ids(k):
        for core in range(n_dp):
            remote(
                ids_ref.at[:, pl.ds(firsts[k], TOK_EDGE)], halo_ids.at[k, p],
                halo_id_send, halo_id_recv, (targets[k], core),
            ).start()

    send_chunk(0)
    for k in range(1, bits):
        pl.semaphore_signal(
            known_sem.at[k - 1], inc=1,
            device_id={"vocab": across(1 << k), "dp": p}, device_id_type=MESH,
        )
        if k == 1:
            mate_copy = remote(
                grad_ref.at[0, :, columns(mate, 0, half)], toks.at[pl.ds(tokens, tokens), :],
                mate_sem.at[0], mate_sem.at[1], (v, mate),
            )
            mate_copy.start()
            mate_id_copy = remote(
                ids_ref, mate_ids, mate_id_sem.at[0], mate_id_sem.at[1], (v, mate)
            )
            mate_id_copy.start()
            send_ids(0)
            table_copy.start()
        pl.semaphore_wait(known_sem.at[k - 1], 1)
    send_ids(1)
    for at in range(1, len(plan)):
        send_chunk(at)

    own_start = v * rows

    def local(ids):
        shifted = ids - own_start
        return jnp.where(shifted < 0, shifted + n_vocab * rows, shifted)

    def onehot(ids, base, count):
        index = lax.broadcasted_iota(jnp.int32, (count, ids.shape[1]), 0) + base
        return jnp.where(ids == index, 1.0, 0.0).astype(jnp.bfloat16)

    def add_squares(values):
        count, wide = values.shape
        lanes = jnp.sum((values * values).reshape(count // 8, 8, wide), axis=0)
        square[...] += functools.reduce(
            jnp.add, [lanes[:, i * 128:(i + 1) * 128] for i in range(wide // 128)]
        )

    square[...] = jnp.zeros_like(square)
    own_id_copy.wait()
    mate_id_copy.wait()
    own_copy.wait()
    mate_copy.wait()

    window_ids = local(jnp.concatenate([own_ids[...], mate_ids[...]], axis=1))
    for block in range(blocks):
        picked = onehot(window_ids, block * EDGE, EDGE)

        @pl.loop(0, half // COLS)
        def _(chunk):
            here = pl.ds(pl.multiple_of(chunk * COLS, COLS), COLS)
            part = jnp.dot(picked, toks[:, here], preferred_element_type=jnp.float32)
            grad[pl.ds(block * EDGE, EDGE), here] = part
            if 0 < block < blocks - 1:
                add_squares(part)

    remote(
        halo_ids, halo_ids, halo_id_send, halo_id_recv, (partner, p)
    ).wait_recv()
    picks = []
    for k in range(2):
        ids = local(jnp.concatenate([halo_ids[k, core] for core in range(n_dp)], axis=1))
        picks.append(onehot(ids, bases[k], EDGE))
    table_copy.wait()
    for at, (k, start, count) in enumerate(plan):
        here = pl.ds(start, count)
        arrived = halo.at[k, :, :, here]
        remote(arrived, arrived, halo_send, halo_recv.at[at], (partner, p)).wait_recv()
        part = jnp.dot(
            picks[k], halo[k, :, :, here].reshape(n_dp * TOK_EDGE, count),
            preferred_element_type=jnp.float32,
        )
        total = grad[pl.ds(bases[k], EDGE), here] + part
        grad[pl.ds(bases[k], EDGE), here] = total
        add_squares(total)

    sums[me] = jnp.sum(square[...], axis=0, keepdims=True)
    for mask in range(n_vocab - 1, -1, -1):
        for core in (mate, p):
            if mask or core is mate:
                remote(
                    sums.at[me], sums.at[me], sum_send, sum_recv, (across(mask), core)
                ).start()
    remote(halo, halo, halo_send, halo_recv.at[0], (partner, p)).wait_send()
    remote(halo_ids, halo_ids, halo_id_send, halo_id_recv, (partner, p)).wait_send()
    others = sums.at[pl.ds(0, n - 1)]
    all_sums = remote(others, others, sum_send, sum_recv, (partner, p))
    all_sums.wait_recv()

    total = jnp.sum(jnp.sum(sums[...], axis=0), axis=1, keepdims=True)
    rms = jnp.sqrt(total / (n_vocab * rows * width))
    clip_scale = 1.0 / jnp.maximum(1.0, rms / norm_limit)
    norm_ref[0:1, :] = jnp.broadcast_to(step_rate * clip_scale, (1, 128))
    norm_ref[1:2, :] = jnp.broadcast_to(rms, (1, 128))
    all_sums.wait_send()


def update(grad, table, norm_ref, out_ref, rms_ref, outbuf, rms_held, out_sem, rms_sem):
    rms_held[0] = norm_ref[1, 0]
    rms_copy = pltpu.make_async_copy(rms_held, rms_ref, rms_sem)
    rms_copy.start()
    rate = norm_ref[0:1, 0:1]
    for block in range(grad.shape[0] // STORE_ROWS):
        here = pl.ds(block * STORE_ROWS, STORE_ROWS)
        moved = table[here, :].astype(jnp.float32) - rate * grad[here, :]
        outbuf[here, :] = moved.astype(jnp.bfloat16)
        pltpu.make_async_copy(outbuf.at[here, :], out_ref.at[here, :], out_sem).start()
    pltpu.make_async_copy(outbuf, out_ref, out_sem).wait()
    rms_copy.wait()


def solution(mesh):
    n_vocab, n_dp = mesh.shape["vocab"], mesh.shape["dp"]
    n = n_vocab * n_dp
    bits = n_vocab.bit_length() - 1

    def body(embed_table, token_ids, grad_rows):
        rows, width = embed_table.shape
        tokens = token_ids.shape[1]
        half = width // n_dp
        plan = chunk_plan(half)
        in_vmem = pl.BlockSpec(memory_space=pltpu.VMEM)
        in_hbm = pl.BlockSpec(memory_space=pltpu.HBM)
        grad, table, norm = pl.pallas_call(
            functools.partial(kernel, (n_vocab, n_dp)),
            name="clipped_update",
            out_shape=(
                jax.ShapeDtypeStruct((rows, half), jnp.float32),
                jax.ShapeDtypeStruct((rows, half), jnp.bfloat16),
                jax.ShapeDtypeStruct((8, 128), jnp.float32),
            ),
            in_specs=[in_hbm, in_hbm, in_hbm],
            out_specs=(in_vmem, in_vmem, in_vmem),
            scratch_shapes=[
                pltpu.VMEM((n_dp * tokens, half), jnp.bfloat16),
                pltpu.VMEM((2, n_dp, TOK_EDGE, half), jnp.bfloat16),
                pltpu.VMEM((n_dp, TOK_EDGE, plan[0][2]), jnp.bfloat16),
                pltpu.VMEM((1, tokens), jnp.int32),
                pltpu.VMEM((1, tokens), jnp.int32),
                pltpu.VMEM((2, n_dp, 1, TOK_EDGE), jnp.int32),
                pltpu.VMEM((8, 128), jnp.float32),
                pltpu.VMEM((n, 1, 128), jnp.float32),
                pltpu.SemaphoreType.DMA,
                pltpu.SemaphoreType.DMA,
                pltpu.SemaphoreType.DMA,
                pltpu.SemaphoreType.DMA((n_dp,)),
                pltpu.SemaphoreType.DMA((2,)),
                pltpu.SemaphoreType.DMA((2,)),
                pltpu.SemaphoreType.DMA,
                pltpu.SemaphoreType.DMA((len(plan),)),
                pltpu.SemaphoreType.DMA,
                pltpu.SemaphoreType.DMA,
                pltpu.SemaphoreType.DMA,
                pltpu.SemaphoreType.DMA,
                pltpu.SemaphoreType.REGULAR((max(bits - 1, 1),)),
            ],
            compiler_params=pltpu.CompilerParams(
                collective_id=0, has_side_effects=True, vmem_limit_bytes=40 * 1024 * 1024
            ),
        )(*(pltpu.with_memory_space_constraint(x, pltpu.HBM) for x in (embed_table, token_ids, grad_rows)))
        updated, grad_rms = pl.pallas_call(
            update,
            name="clipped_step",
            out_shape=(
                jax.ShapeDtypeStruct((rows, half), jnp.bfloat16),
                jax.ShapeDtypeStruct((1,), jnp.float32),
            ),
            in_specs=[in_vmem, in_vmem, in_vmem],
            out_specs=(in_hbm, in_hbm),
            scratch_shapes=[
                pltpu.VMEM((rows, half), jnp.bfloat16),
                pltpu.SMEM((1,), jnp.float32),
                pltpu.SemaphoreType.DMA,
                pltpu.SemaphoreType.DMA,
            ],
            compiler_params=pltpu.CompilerParams(vmem_limit_bytes=24 * 1024 * 1024),
        )(grad, table, norm)
        return updated, grad_rms

    in_specs = (P("vocab", None), P("dp", "vocab"), P("dp", "vocab", None))
    out_specs = (P("vocab", "dp"), P())
    return jax.shard_map(body, mesh=mesh, in_specs=in_specs, out_specs=out_specs, check_vma=False)
```

```python
import functools

import jax
import jax.numpy as jnp
from jax import lax
from jax.experimental import pallas as pl
from jax.experimental.pallas import tpu as pltpu
from jax.sharding import PartitionSpec as P

MESH = pl.DeviceIdType.MESH
TOK_EDGE = 128
EDGE = 256
COLS = 512
STORE_ROWS = 16
STORE_COLS = 256

step_rate = 0.5
norm_limit = 1.0


RELAYED = ((4, 0), (4, 1))
RELAY_FROM = (2, 3)


def chunk_plan(half):
    quarter = half // 4
    narrow = 128
    return (
        (0, 0, quarter),
        (0, quarter, 2 * narrow),
        (1, 0, 2 * quarter),
        (1, 2 * quarter, 2 * quarter),
        (0, quarter + 2 * narrow, narrow),
        (0, quarter + 3 * narrow, narrow),
        (0, 2 * quarter, quarter),
        (0, 3 * quarter, quarter - narrow),
        (0, half - narrow, narrow),
    )


def kernel(sizes, table_ref, ids_ref, grad_ref, grad, table, norm_ref,
           toks, halo, stage, relayed, own_ids, mate_ids, halo_ids, square, sums,
           own_sem, own_id_sem, table_sem, stage_sem, mate_sem, mate_id_sem,
           halo_send, halo_recv, halo_id_send, halo_id_recv, sum_send, sum_recv,
           relay_send, relay_recv, known_sem):
    n_vocab, n_dp = sizes
    rows, width = table_ref.shape
    tokens = ids_ref.shape[1]
    half = width // n_dp
    n = n_vocab * n_dp
    blocks = rows // EDGE
    bits = n_vocab.bit_length() - 1
    plan = chunk_plan(half)
    v = lax.axis_index("vocab")
    p = lax.axis_index("dp")
    me = v * n_dp + p
    mate = 1 - p
    odd = lax.rem(v, 2)
    below = lax.rem(v + n_vocab - 1, n_vocab)
    above = lax.rem(v + 1, n_vocab)
    set_bits = [lax.rem(v // (1 << k), 2) for k in range(bits)]
    steps = [(1 << k) - 2 * (1 << k) * set_bits[k] for k in range(bits)]
    zone = v // (n_vocab // 4)

    def across(mask):
        return functools.reduce(lambda a, b: a + b, [steps[k] for k in range(bits) if mask >> k & 1], v)

    partner = across(1)
    opposite = across(3 * n_vocab // 4)
    beyond = across(3 * n_vocab // 4 + 1)
    far = jnp.where(odd == 1, above, below)
    last = tokens - TOK_EDGE
    targets = (partner, far)
    firsts = tuple(
        pl.multiple_of(first, TOK_EDGE) for first in ((1 - odd) * last, odd * last)
    )
    bases = tuple(
        pl.multiple_of(base, EDGE) for base in ((1 - odd) * (rows - EDGE), odd * (rows - EDGE))
    )

    def columns(core, start, count):
        return pl.ds(pl.multiple_of(core * half + start, 128), count)

    def remote(src, dst, send, recv, device):
        return pltpu.make_async_remote_copy(
            src_ref=src, dst_ref=dst, send_sem=send, recv_sem=recv,
            device_id={"vocab": device[0], "dp": device[1]}, device_id_type=MESH,
        )

    stage_copies = [
        pltpu.make_async_copy(
            grad_ref.at[0, pl.ds(firsts[0], TOK_EDGE), pl.ds(core * half, plan[0][2])],
            stage.at[core], stage_sem.at[core],
        )
        for core in range(n_dp)
    ]
    for copy in stage_copies:
        copy.start()
    barrier = pltpu.get_barrier_semaphore()

    def greet(w, core):
        pl.semaphore_signal(
            barrier, inc=1, device_id={"vocab": w, "dp": core}, device_id_type=MESH
        )

    for core in range(n_dp):
        greet(partner, core)
    greet(v, mate)
    greet(across(2), p)
    for k in range(2, bits):
        pl.when(set_bits[k] == 0)(functools.partial(greet, across(1 << k), p))
    pl.when(zone < 2)(functools.partial(greet, beyond, p))
    awaited = n_dp + 2 + sum(set_bits[2:]) + zone // 2
    own_half = pl.ds(pl.multiple_of(p * half, half), half)
    own_copy = pltpu.make_async_copy(
        grad_ref.at[0, :, own_half], toks.at[pl.ds(0, tokens), :], own_sem
    )
    own_copy.start()
    own_id_copy = pltpu.make_async_copy(ids_ref, own_ids, own_id_sem)
    own_id_copy.start()
    table_copy = pltpu.make_async_copy(table_ref.at[:, own_half], table, table_sem)
    for copy in stage_copies:
        copy.wait()
    pl.semaphore_wait(barrier, awaited)

    def source(at, core):
        k, start, count = plan[at]
        return grad_ref.at[0, pl.ds(firsts[k], TOK_EDGE), pl.ds(core * half + start, count)]

    def place(at):
        k, start, count = plan[at]
        return halo.at[k, p, :, pl.ds(start, count)]

    def send_chunk(at):
        for core in range(n_dp):
            copy = remote(
                stage.at[core] if at == 0 else source(at, core), place(at),
                halo_send, halo_recv.at[at], (targets[plan[at][0]], core),
            )
            if (at, core) in RELAYED:
                pl.when(zone < RELAY_FROM[RELAYED.index((at, core))])(copy.start)
            else:
                copy.start()

    def relay_units(count):
        return remote(
            relayed.at[pl.ds(0, count)], relayed.at[pl.ds(0, count)],
            relay_send, relay_recv, (opposite, p),
        )

    def send_ids(k):
        for core in range(n_dp):
            remote(
                ids_ref.at[:, pl.ds(firsts[k], TOK_EDGE)], halo_ids.at[k, p],
                halo_id_send, halo_id_recv, (targets[k], core),
            ).start()

    for unit, (at, core) in enumerate(RELAYED):
        copy = remote(
            source(at, core), relayed.at[unit], halo_send, relay_recv, (beyond, p)
        )
        pl.when(zone >= RELAY_FROM[unit])(copy.start)
    send_chunk(0)
    send_chunk(1)
    mate_copy = remote(
        grad_ref.at[0, :, columns(mate, 0, half)], toks.at[pl.ds(tokens, tokens), :],
        mate_sem.at[0], mate_sem.at[1], (v, mate),
    )
    mate_copy.start()
    mate_id_copy = remote(
        ids_ref, mate_ids, mate_id_sem.at[0], mate_id_sem.at[1], (v, mate)
    )
    mate_id_copy.start()
    send_ids(0)
    table_copy.start()

    def tell(k):
        pl.semaphore_signal(
            known_sem.at[k - 1], inc=1,
            device_id={"vocab": across(1 << k), "dp": p}, device_id_type=MESH,
        )

    for k in range(1, bits):
        if k == 1:
            tell(k)
        else:
            pl.when(set_bits[k] == 1)(functools.partial(tell, k))
        pl.semaphore_wait(known_sem.at[k - 1], 1)
        if k > 1:
            pl.when(set_bits[k] == 0)(functools.partial(tell, k))
    send_ids(1)

    for owner in range(2):
        units = [unit for unit in range(len(RELAYED)) if RELAY_FROM[unit] <= 3 - owner]

        @pl.when(zone == owner)
        def _():
            relay_units(len(units)).wait_recv()
            for unit in units:
                at, core = RELAYED[unit]
                remote(
                    relayed.at[unit], place(at), relay_send, halo_recv.at[at], (opposite, core)
                ).start()

    for at in range(2, len(plan)):
        send_chunk(at)

    own_start = v * rows

    def local(ids):
        shifted = ids - own_start
        return jnp.where(shifted < 0, shifted + n_vocab * rows, shifted)

    def onehot(ids, base, count):
        index = lax.broadcasted_iota(jnp.int32, (count, ids.shape[1]), 0) + base
        return jnp.where(ids == index, 1.0, 0.0).astype(jnp.bfloat16)

    def add_squares(values):
        count, wide = values.shape
        lanes = jnp.sum((values * values).reshape(count // 8, 8, wide), axis=0)
        square[...] += functools.reduce(
            jnp.add, [lanes[:, i * 128:(i + 1) * 128] for i in range(wide // 128)]
        )

    square[...] = jnp.zeros_like(square)
    own_id_copy.wait()
    mate_id_copy.wait()
    own_copy.wait()
    mate_copy.wait()

    window_ids = local(jnp.concatenate([own_ids[...], mate_ids[...]], axis=1))
    for block in range(blocks):
        picked = onehot(window_ids, block * EDGE, EDGE)

        @pl.loop(0, half // COLS)
        def _(chunk):
            here = pl.ds(pl.multiple_of(chunk * COLS, COLS), COLS)
            part = jnp.dot(picked, toks[:, here], preferred_element_type=jnp.float32)
            grad[pl.ds(block * EDGE, EDGE), here] = part
            if 0 < block < blocks - 1:
                add_squares(part)

    remote(halo_ids, halo_ids, halo_id_send, halo_id_recv, (partner, p)).wait_recv()
    picks = []
    for k in range(2):
        ids = local(jnp.concatenate([halo_ids[k, core] for core in range(n_dp)], axis=1))
        picks.append(onehot(ids, bases[k], EDGE))
    table_copy.wait()
    for at, (k, start, count) in enumerate(plan):
        here = pl.ds(start, count)
        arrived = halo.at[k, :, :, here]
        remote(arrived, arrived, halo_send, halo_recv.at[at], (partner, p)).wait_recv()
        part = jnp.dot(
            picks[k], halo[k, :, :, here].reshape(n_dp * TOK_EDGE, count),
            preferred_element_type=jnp.float32,
        )
        total = grad[pl.ds(bases[k], EDGE), here] + part
        grad[pl.ds(bases[k], EDGE), here] = total
        add_squares(total)

    sums[me] = jnp.sum(square[...], axis=0, keepdims=True)
    for w in range(n_vocab):
        for core in range(n_dp):
            copy = remote(sums.at[me], sums.at[me], sum_send, sum_recv, (w, core))
            pl.when(me != w * n_dp + core)(copy.start)
    remote(halo, halo, halo_send, halo_recv.at[0], (partner, p)).wait_send()
    remote(halo_ids, halo_ids, halo_id_send, halo_id_recv, (partner, p)).wait_send()
    for owner in range(2):
        count = sum(start <= 3 - owner for start in RELAY_FROM)
        pl.when(zone == owner)(relay_units(count).wait_send)
    others = sums.at[pl.ds(0, n - 1)]
    all_sums = remote(others, others, sum_send, sum_recv, (partner, p))
    all_sums.wait_recv()

    total = jnp.sum(jnp.sum(sums[...], axis=0), axis=1, keepdims=True)
    rms = jnp.sqrt(total / (n_vocab * rows * width))
    clip_scale = 1.0 / jnp.maximum(1.0, rms / norm_limit)
    norm_ref[0:1, :] = jnp.broadcast_to(step_rate * clip_scale, (1, 128))
    norm_ref[1:2, :] = jnp.broadcast_to(rms, (1, 128))
    all_sums.wait_send()


def update(grad, table, norm_ref, out_ref, rms_ref, outbuf, rms_held, out_sem, rms_sem):
    rms_held[0] = norm_ref[1, 0]
    rms_copy = pltpu.make_async_copy(rms_held, rms_ref, rms_sem)
    rms_copy.start()
    rate = norm_ref[0:1, 0:1]
    for block in range(grad.shape[0] // STORE_ROWS):
        here = pl.ds(block * STORE_ROWS, STORE_ROWS)
        for start in range(0, grad.shape[1], STORE_COLS):
            at = (here, pl.ds(start, STORE_COLS))
            moved = table[at].astype(jnp.float32) - rate * grad[at]
            outbuf[at] = moved.astype(jnp.bfloat16)
        pltpu.make_async_copy(outbuf.at[here, :], out_ref.at[here, :], out_sem).start()
    pltpu.make_async_copy(outbuf, out_ref, out_sem).wait()
    rms_copy.wait()


def solution(mesh):
    n_vocab, n_dp = mesh.shape["vocab"], mesh.shape["dp"]
    n = n_vocab * n_dp
    bits = n_vocab.bit_length() - 1

    def body(embed_table, token_ids, grad_rows):
        rows, width = embed_table.shape
        tokens = token_ids.shape[1]
        half = width // n_dp
        plan = chunk_plan(half)
        in_vmem = pl.BlockSpec(memory_space=pltpu.VMEM)
        in_hbm = pl.BlockSpec(memory_space=pltpu.HBM)
        grad, table, norm = pl.pallas_call(
            functools.partial(kernel, (n_vocab, n_dp)),
            name="clipped_update",
            out_shape=(
                jax.ShapeDtypeStruct((rows, half), jnp.float32),
                jax.ShapeDtypeStruct((rows, half), jnp.bfloat16),
                jax.ShapeDtypeStruct((8, 128), jnp.float32),
            ),
            in_specs=[in_hbm, in_hbm, in_hbm],
            out_specs=(in_vmem, in_vmem, in_vmem),
            scratch_shapes=[
                pltpu.VMEM((n_dp * tokens, half), jnp.bfloat16),
                pltpu.VMEM((2, n_dp, TOK_EDGE, half), jnp.bfloat16),
                pltpu.VMEM((n_dp, TOK_EDGE, plan[0][2]), jnp.bfloat16),
                pltpu.VMEM((len(RELAYED), TOK_EDGE, plan[RELAYED[0][0]][2]), jnp.bfloat16),
                pltpu.VMEM((1, tokens), jnp.int32),
                pltpu.VMEM((1, tokens), jnp.int32),
                pltpu.VMEM((2, n_dp, 1, TOK_EDGE), jnp.int32),
                pltpu.VMEM((8, 128), jnp.float32),
                pltpu.VMEM((n, 1, 128), jnp.float32),
                pltpu.SemaphoreType.DMA,
                pltpu.SemaphoreType.DMA,
                pltpu.SemaphoreType.DMA,
                pltpu.SemaphoreType.DMA((n_dp,)),
                pltpu.SemaphoreType.DMA((2,)),
                pltpu.SemaphoreType.DMA((2,)),
                pltpu.SemaphoreType.DMA,
                pltpu.SemaphoreType.DMA((len(plan),)),
                pltpu.SemaphoreType.DMA,
                pltpu.SemaphoreType.DMA,
                pltpu.SemaphoreType.DMA,
                pltpu.SemaphoreType.DMA,
                pltpu.SemaphoreType.DMA,
                pltpu.SemaphoreType.DMA,
                pltpu.SemaphoreType.REGULAR((max(bits - 1, 1),)),
            ],
            compiler_params=pltpu.CompilerParams(
                collective_id=0, has_side_effects=True, vmem_limit_bytes=40 * 1024 * 1024
            ),
        )(*(pltpu.with_memory_space_constraint(x, pltpu.HBM) for x in (embed_table, token_ids, grad_rows)))
        updated, grad_rms = pl.pallas_call(
            update,
            name="clipped_step",
            out_shape=(
                jax.ShapeDtypeStruct((rows, half), jnp.bfloat16),
                jax.ShapeDtypeStruct((1,), jnp.float32),
            ),
            in_specs=[in_vmem, in_vmem, in_vmem],
            out_specs=(in_hbm, in_hbm),
            scratch_shapes=[
                pltpu.VMEM((rows, half), jnp.bfloat16),
                pltpu.SMEM((1,), jnp.float32),
                pltpu.SemaphoreType.DMA,
                pltpu.SemaphoreType.DMA,
            ],
            compiler_params=pltpu.CompilerParams(vmem_limit_bytes=24 * 1024 * 1024),
        )(grad, table, norm)
        return updated, grad_rms

    in_specs = (P("vocab", None), P("dp", "vocab"), P("dp", "vocab", None))
    out_specs = (P("vocab", "dp"), P())
    return jax.shard_map(body, mesh=mesh, in_specs=in_specs, out_specs=out_specs, check_vma=False)
```

```python
import functools

import jax
import jax.numpy as jnp
from jax import lax
from jax.experimental import pallas as pl
from jax.experimental.pallas import tpu as pltpu
from jax.sharding import PartitionSpec as P

MESH = pl.DeviceIdType.MESH
TOK_EDGE = 128
EDGE = 256
COLS = 512
STORE_ROWS = 16
STORE_COLS = 256

step_rate = 0.5
norm_limit = 1.0


PIECE = 512

RELAYED = {
    (2, 0, 0): ((0, 3, 0),),
    (2, 1, 0): ((0, 3, 0),),
    (3, 0, 0): ((0, 3, 0), (1, 3, 1)),
    (3, 0, 1): ((0, 3, 0), (1, 3, 1)),
    (3, 1, 0): ((0, 3, 0), (1, 3, 1)),
    (3, 1, 1): ((0, 3, 0), (1, 3, 1)),
}
SLOTS = 2
FAR_NARROW = 8
FAR_RELAYED = {(0, 0): 1, (0, 1): 1, (1, 0): 1, (1, 1): 1, (2, 0): 1, (3, 0): 1}


def chunk_plan(half):
    quarter = half // 4
    narrow = 128
    return (
        (0, 0, quarter, 0),
        (0, quarter, 2 * narrow, 0),
        (1, 0, half - narrow, 1),
        (0, quarter + 2 * narrow, narrow, 2),
        (0, quarter + 3 * narrow, narrow, 3),
        (0, 2 * quarter, quarter, 4),
        (0, 3 * quarter, quarter - narrow, 5),
        (0, half - narrow, narrow, 7),
        (1, half - narrow, narrow, 6),
    )


def groups_of(plan):
    groups = {}
    for k, start, count, group in plan:
        first = groups.get(group, (k, start, 0))
        groups[group] = (k, first[1], first[2] + count)
    return [groups[group] for group in sorted(groups)]


def kernel(sizes, table_ref, ids_ref, grad_ref, grad, table, norm_ref,
           toks, halo, stage, relayed, own_ids, mate_ids, halo_ids, square, sums,
           own_sem, own_id_sem, table_sem, stage_sem, mate_sem, mate_id_sem,
           halo_send, halo_recv, halo_id_send, halo_id_recv, sum_send, sum_recv,
           relay_send, relay_recv, far_send, far_recv, known_sem):
    n_vocab, n_dp = sizes
    rows, width = table_ref.shape
    tokens = ids_ref.shape[1]
    half = width // n_dp
    n = n_vocab * n_dp
    blocks = rows // EDGE
    bits = n_vocab.bit_length() - 1
    plan = chunk_plan(half)
    v = lax.axis_index("vocab")
    p = lax.axis_index("dp")
    me = v * n_dp + p
    mate = 1 - p
    odd = lax.rem(v, 2)
    below = lax.rem(v + n_vocab - 1, n_vocab)
    above = lax.rem(v + 1, n_vocab)
    set_bits = [lax.rem(v // (1 << k), 2) for k in range(bits)]
    steps = [(1 << k) - 2 * (1 << k) * set_bits[k] for k in range(bits)]
    zone = v // (n_vocab // 4)
    top = 3 * n_vocab // 4

    def across(mask):
        return functools.reduce(lambda a, b: a + b, [steps[k] for k in range(bits) if mask >> k & 1], v)

    partner = across(1)
    far = jnp.where(odd == 1, above, below)
    last = tokens - TOK_EDGE
    targets = (partner, far)
    firsts = tuple(
        pl.multiple_of(first, TOK_EDGE) for first in ((1 - odd) * last, odd * last)
    )
    bases = tuple(
        pl.multiple_of(base, EDGE) for base in ((1 - odd) * (rows - EDGE), odd * (rows - EDGE))
    )

    def columns(core, start, count):
        return pl.ds(pl.multiple_of(core * half + start, 128), count)

    def remote(src, dst, send, recv, device):
        return pltpu.make_async_remote_copy(
            src_ref=src, dst_ref=dst, send_sem=send, recv_sem=recv,
            device_id={"vocab": device[0], "dp": device[1]}, device_id_type=MESH,
        )

    barrier = pltpu.get_barrier_semaphore()

    def greet(w, core):
        pl.semaphore_signal(
            barrier, inc=1, device_id={"vocab": w, "dp": core}, device_id_type=MESH
        )

    def at_place(quarter, second, core=None):
        here = jnp.logical_and(zone == quarter, set_bits[1] == second)
        return here if core is None else jnp.logical_and(here, p == core)

    relay = across(top + 1)
    beyond = across(top)
    via = far + jnp.where(odd == 1, 1, -1)
    far_quarter = far // (n_vocab // 4)

    for core in range(n_dp):
        greet(partner, core)
    greet(v, mate)
    stage_copies = [
        pltpu.make_async_copy(
            grad_ref.at[0, pl.ds(firsts[0], TOK_EDGE), pl.ds(core * half, plan[0][2])],
            stage.at[core], stage_sem,
        )
        for core in range(n_dp)
    ]
    for copy in stage_copies:
        copy.start()
    for k in range(1, bits):
        pl.when(set_bits[k] == 0)(functools.partial(greet, across(1 << k), p))
    awaited = n_dp + 1 + sum(set_bits[1:])
    for quarter, second in sorted({key[:2] for key in RELAYED}):
        pl.when(at_place(3 - quarter, second))(functools.partial(greet, relay, p))
        awaited += at_place(quarter, second).astype(jnp.int32)
    own_half = pl.ds(pl.multiple_of(p * half, half), half)
    own_copy = pltpu.make_async_copy(
        grad_ref.at[0, :, own_half], toks.at[pl.ds(0, tokens), :], own_sem
    )
    own_copy.start()
    own_id_copy = pltpu.make_async_copy(ids_ref, own_ids, own_id_sem)
    own_id_copy.start()
    table_copy = pltpu.make_async_copy(table_ref.at[:, own_half], table, table_sem)
    pltpu.make_async_copy(stage, stage, stage_sem).wait()
    pl.semaphore_wait(barrier, awaited)

    def source(at, core):
        k, start, count, _ = plan[at]
        return grad_ref.at[0, pl.ds(firsts[k], TOK_EDGE), pl.ds(core * half + start, count)]

    def place(at):
        k, start, count, _ = plan[at]
        return halo.at[k, p, :, pl.ds(start, count)]

    def send_chunk(at):
        k, _, _, group = plan[at]
        for core in range(n_dp):
            copy = remote(
                stage.at[core] if at == 0 else source(at, core), place(at),
                halo_send, halo_recv.at[group], (targets[k], core),
            )
            around = [
                at_place(*key) for key, flows in RELAYED.items()
                if (at, core) in [flow[1:3] for flow in flows]
            ]
            if at == FAR_NARROW:
                around = [by_way(*key) for key, count in FAR_RELAYED.items() if core < count]
            if around:
                pl.when(jnp.logical_not(functools.reduce(jnp.logical_or, around)))(copy.start)
            else:
                copy.start()

    def relay_slots(first, count, send, recv):
        slots = relayed.at[pl.ds(first, count)]
        return remote(slots, slots, send, recv, (partner, p))

    def by_way(quarter, core):
        here = jnp.logical_and(far_quarter == quarter, set_bits[1] == 1)
        return jnp.logical_and(here, p == core)

    def send_ids(k):
        for core in range(n_dp):
            remote(
                ids_ref.at[:, pl.ds(firsts[k], TOK_EDGE)], halo_ids.at[k, p],
                halo_id_send, halo_id_recv, (targets[k], core),
            ).start()

    for key, flows in RELAYED.items():
        @pl.when(at_place(*key))
        def _():
            for slot, at, core in flows:
                remote(
                    source(at, core), relayed.at[slot], halo_send, relay_recv, (relay, p)
                ).start()

    send_chunk(0)
    send_chunk(1)
    mate_copy = remote(
        grad_ref.at[0, :, columns(mate, 0, half)], toks.at[pl.ds(tokens, tokens), :],
        mate_sem.at[0], mate_sem.at[1], (v, mate),
    )
    mate_copy.start()
    mate_id_copy = remote(
        ids_ref, mate_ids, mate_id_sem.at[0], mate_id_sem.at[1], (v, mate)
    )
    mate_id_copy.start()
    send_ids(0)
    table_copy.start()

    def tell(k):
        pl.semaphore_signal(
            known_sem.at[k - 1], inc=1,
            device_id={"vocab": across(1 << k), "dp": p}, device_id_type=MESH,
        )

    for k in range(1, bits):
        pl.when(set_bits[k] == 1)(functools.partial(tell, k))
        pl.semaphore_wait(known_sem.at[k - 1], 1)
        pl.when(set_bits[k] == 0)(functools.partial(tell, k))
    send_ids(1)

    for key, count in FAR_RELAYED.items():
        @pl.when(by_way(*key))
        def _():
            for core in range(count):
                remote(
                    source(FAR_NARROW, core), relayed.at[SLOTS + core], halo_send, far_recv, (via, p)
                ).start()

    for at in (2, FAR_NARROW, 3, 4, 5):
        send_chunk(at)
    for (quarter, second, core), flows in RELAYED.items():
        @pl.when(at_place(3 - quarter, second, core))
        def _():
            relay_slots(0, len(flows), relay_send, relay_recv).wait_recv()
            for slot, at, target in flows:
                remote(
                    relayed.at[slot], place(at), relay_send, halo_recv.at[plan[at][3]],
                    (beyond, target),
                ).start()

    def forward_far():
        for (quarter, core), count in FAR_RELAYED.items():
            @pl.when(at_place(quarter, 0, core))
            def _():
                relay_slots(SLOTS, count, far_send, far_recv).wait_recv()
                for target in range(count):
                    remote(
                        relayed.at[SLOTS + target], place(FAR_NARROW), far_send,
                        halo_recv.at[plan[FAR_NARROW][3]], (partner, target),
                    ).start()

    own_start = v * rows

    def local(ids):
        shifted = ids - own_start
        return jnp.where(shifted < 0, shifted + n_vocab * rows, shifted)

    def onehot(ids, base, count):
        index = lax.broadcasted_iota(jnp.int32, (count, ids.shape[1]), 0) + base
        return jnp.where(ids == index, 1.0, 0.0).astype(jnp.bfloat16)

    def add_squares(values):
        count, wide = values.shape
        lanes = jnp.sum((values * values).reshape(count // 8, 8, wide), axis=0)
        square[...] += functools.reduce(
            jnp.add, [lanes[:, i * 128:(i + 1) * 128] for i in range(wide // 128)]
        )

    square[...] = jnp.zeros_like(square)
    own_id_copy.wait()
    mate_id_copy.wait()
    own_copy.wait()
    mate_copy.wait()

    window_ids = local(jnp.concatenate([own_ids[...], mate_ids[...]], axis=1))
    for block in range(blocks):
        if block == 1:
            forward_far()
            for at in (6, 7):
                send_chunk(at)
        picked = onehot(window_ids, block * EDGE, EDGE)

        @pl.loop(0, half // COLS)
        def _(chunk):
            here = pl.ds(pl.multiple_of(chunk * COLS, COLS), COLS)
            part = jnp.dot(picked, toks[:, here], preferred_element_type=jnp.float32)
            grad[pl.ds(block * EDGE, EDGE), here] = part
            if 0 < block < blocks - 1:
                add_squares(part)

    remote(halo_ids, halo_ids, halo_id_send, halo_id_recv, (partner, p)).wait_recv()
    picks = []
    for k in range(2):
        ids = local(jnp.concatenate([halo_ids[k, core] for core in range(n_dp)], axis=1))
        picks.append(onehot(ids, bases[k], EDGE))
    table_copy.wait()
    for group, (k, first, size) in enumerate(groups_of(plan)):
        arrived = halo.at[k, :, :, pl.ds(first, size)]
        remote(arrived, arrived, halo_send, halo_recv.at[group], (partner, p)).wait_recv()
        for start in range(first, first + size, PIECE):
            count = min(PIECE, first + size - start)
            here = pl.ds(start, count)
            part = jnp.dot(
                picks[k], halo[k, :, :, here].reshape(n_dp * TOK_EDGE, count),
                preferred_element_type=jnp.float32,
            )
            total = grad[pl.ds(bases[k], EDGE), here] + part
            grad[pl.ds(bases[k], EDGE), here] = total
            add_squares(total)

    sums[me] = jnp.sum(square[...], axis=0, keepdims=True)
    for w in range(n_vocab):
        for core in range(n_dp):
            copy = remote(sums.at[me], sums.at[me], sum_send, sum_recv, (w, core))
            pl.when(me != w * n_dp + core)(copy.start)
    remote(halo, halo, halo_send, halo_recv.at[0], (partner, p)).wait_send()
    remote(halo_ids, halo_ids, halo_id_send, halo_id_recv, (partner, p)).wait_send()
    for (quarter, second, core), flows in RELAYED.items():
        pl.when(at_place(3 - quarter, second, core))(
            relay_slots(0, len(flows), relay_send, relay_recv).wait_send
        )
    for (quarter, core), count in FAR_RELAYED.items():
        pl.when(at_place(quarter, 0, core))(
            relay_slots(SLOTS, count, far_send, far_recv).wait_send
        )
    others = sums.at[pl.ds(0, n - 1)]
    all_sums = remote(others, others, sum_send, sum_recv, (partner, p))
    all_sums.wait_recv()

    total = jnp.sum(jnp.sum(sums[...], axis=0), axis=1, keepdims=True)
    rms = jnp.sqrt(total / (n_vocab * rows * width))
    clip_scale = 1.0 / jnp.maximum(1.0, rms / norm_limit)
    norm_ref[0:1, :] = jnp.broadcast_to(step_rate * clip_scale, (1, 128))
    norm_ref[1:2, :] = jnp.broadcast_to(rms, (1, 128))
    all_sums.wait_send()


def update(grad, table, norm_ref, out_ref, rms_ref, outbuf, rms_held, out_sem, rms_sem):
    rms_held[0] = norm_ref[1, 0]
    rms_copy = pltpu.make_async_copy(rms_held, rms_ref, rms_sem)
    rms_copy.start()
    rate = norm_ref[0:1, 0:1]
    for block in range(grad.shape[0] // STORE_ROWS):
        here = pl.ds(block * STORE_ROWS, STORE_ROWS)
        for start in range(0, grad.shape[1], STORE_COLS):
            at = (here, pl.ds(start, STORE_COLS))
            moved = table[at].astype(jnp.float32) - rate * grad[at]
            outbuf[at] = moved.astype(jnp.bfloat16)
        pltpu.make_async_copy(outbuf.at[here, :], out_ref.at[here, :], out_sem).start()
    pltpu.make_async_copy(outbuf, out_ref, out_sem).wait()
    rms_copy.wait()


def solution(mesh):
    n_vocab, n_dp = mesh.shape["vocab"], mesh.shape["dp"]
    n = n_vocab * n_dp
    bits = n_vocab.bit_length() - 1

    def body(embed_table, token_ids, grad_rows):
        rows, width = embed_table.shape
        tokens = token_ids.shape[1]
        half = width // n_dp
        plan = chunk_plan(half)
        in_vmem = pl.BlockSpec(memory_space=pltpu.VMEM)
        in_hbm = pl.BlockSpec(memory_space=pltpu.HBM)
        grad, table, norm = pl.pallas_call(
            functools.partial(kernel, (n_vocab, n_dp)),
            name="clipped_update",
            out_shape=(
                jax.ShapeDtypeStruct((rows, half), jnp.float32),
                jax.ShapeDtypeStruct((rows, half), jnp.bfloat16),
                jax.ShapeDtypeStruct((8, 128), jnp.float32),
            ),
            in_specs=[in_hbm, in_hbm, in_hbm],
            out_specs=(in_vmem, in_vmem, in_vmem),
            scratch_shapes=[
                pltpu.VMEM((n_dp * tokens, half), jnp.bfloat16),
                pltpu.VMEM((2, n_dp, TOK_EDGE, half), jnp.bfloat16),
                pltpu.VMEM((n_dp, TOK_EDGE, plan[0][2]), jnp.bfloat16),
                pltpu.VMEM((SLOTS + max(FAR_RELAYED.values()), TOK_EDGE, 128), jnp.bfloat16),
                pltpu.VMEM((1, tokens), jnp.int32),
                pltpu.VMEM((1, tokens), jnp.int32),
                pltpu.VMEM((2, n_dp, 1, TOK_EDGE), jnp.int32),
                pltpu.VMEM((8, 128), jnp.float32),
                pltpu.VMEM((n, 1, 128), jnp.float32),
                pltpu.SemaphoreType.DMA,
                pltpu.SemaphoreType.DMA,
                pltpu.SemaphoreType.DMA,
                pltpu.SemaphoreType.DMA,
                pltpu.SemaphoreType.DMA((2,)),
                pltpu.SemaphoreType.DMA((2,)),
                pltpu.SemaphoreType.DMA,
                pltpu.SemaphoreType.DMA((len(groups_of(plan)),)),
                pltpu.SemaphoreType.DMA,
                pltpu.SemaphoreType.DMA,
                pltpu.SemaphoreType.DMA,
                pltpu.SemaphoreType.DMA,
                pltpu.SemaphoreType.DMA,
                pltpu.SemaphoreType.DMA,
                pltpu.SemaphoreType.DMA,
                pltpu.SemaphoreType.DMA,
                pltpu.SemaphoreType.REGULAR((max(bits - 1, 1),)),
            ],
            compiler_params=pltpu.CompilerParams(
                collective_id=0, has_side_effects=True, vmem_limit_bytes=40 * 1024 * 1024
            ),
        )(*(pltpu.with_memory_space_constraint(x, pltpu.HBM) for x in (embed_table, token_ids, grad_rows)))
        updated, grad_rms = pl.pallas_call(
            update,
            name="clipped_step",
            out_shape=(
                jax.ShapeDtypeStruct((rows, half), jnp.bfloat16),
                jax.ShapeDtypeStruct((1,), jnp.float32),
            ),
            in_specs=[in_vmem, in_vmem, in_vmem],
            out_specs=(in_hbm, in_hbm),
            scratch_shapes=[
                pltpu.VMEM((rows, half), jnp.bfloat16),
                pltpu.SMEM((1,), jnp.float32),
                pltpu.SemaphoreType.DMA,
                pltpu.SemaphoreType.DMA,
            ],
            compiler_params=pltpu.CompilerParams(vmem_limit_bytes=24 * 1024 * 1024),
        )(grad, table, norm)
        return updated, grad_rms

    in_specs = (P("vocab", None), P("dp", "vocab"), P("dp", "vocab", None))
    out_specs = (P("vocab", "dp"), P())
    return jax.shard_map(body, mesh=mesh, in_specs=in_specs, out_specs=out_specs, check_vma=False)
```

```python
import functools

import jax
import jax.numpy as jnp
from jax import lax
from jax.experimental import pallas as pl
from jax.experimental.pallas import tpu as pltpu
from jax.sharding import PartitionSpec as P

MESH = pl.DeviceIdType.MESH
TOK_EDGE = 128
EDGE = 256
COLS = 512
STORE_ROWS = 16
STORE_COLS = 256

step_rate = 0.5
norm_limit = 1.0


PIECE = 512

RELAYED = {
    (2, 0, 0): ((0, 3, 0),),
    (2, 1, 0): ((0, 3, 0),),
    (3, 0, 0): ((0, 3, 0), (1, 3, 1)),
    (3, 0, 1): ((0, 3, 0), (1, 3, 1)),
    (3, 1, 0): ((0, 3, 0), (1, 3, 1)),
    (3, 1, 1): ((0, 3, 0), (1, 3, 1)),
}
SLOTS = 2
FAR_NARROW = 8
FAR_RELAYED = {(0, 0): 1, (0, 1): 1, (1, 0): 1, (1, 1): 1, (2, 0): 1, (3, 0): 1}


def chunk_plan(half):
    quarter = half // 4
    narrow = 128
    return (
        (0, 0, quarter, 0),
        (0, quarter, 2 * narrow, 0),
        (1, 0, half - narrow, 1),
        (0, quarter + 2 * narrow, narrow, 2),
        (0, quarter + 3 * narrow, narrow, 3),
        (0, 2 * quarter, 2 * quarter - 2 * narrow, 4),
        (0, half - 2 * narrow, narrow, 5),
        (0, half - narrow, narrow, 7),
        (1, half - narrow, narrow, 6),
    )


def groups_of(plan):
    groups = {}
    for k, start, count, group in plan:
        first = groups.get(group, (k, start, 0))
        groups[group] = (k, first[1], first[2] + count)
    return [groups[group] for group in sorted(groups)]


def kernel(sizes, table_ref, ids_ref, grad_ref, grad, table, norm_ref,
           toks, halo, stage, relayed, own_ids, mate_ids, halo_ids, square, sums,
           own_sem, own_id_sem, table_sem, stage_sem, mate_sem, mate_id_sem,
           halo_send, halo_recv, halo_id_send, halo_id_recv, sum_send, sum_recv,
           relay_send, relay_recv, far_send, far_recv, known_sem):
    n_vocab, n_dp = sizes
    rows, width = table_ref.shape
    tokens = ids_ref.shape[1]
    half = width // n_dp
    n = n_vocab * n_dp
    blocks = rows // EDGE
    bits = n_vocab.bit_length() - 1
    plan = chunk_plan(half)
    v = lax.axis_index("vocab")
    p = lax.axis_index("dp")
    me = v * n_dp + p
    mate = 1 - p
    odd = lax.rem(v, 2)
    below = lax.rem(v + n_vocab - 1, n_vocab)
    above = lax.rem(v + 1, n_vocab)
    set_bits = [lax.rem(v // (1 << k), 2) for k in range(bits)]
    steps = [(1 << k) - 2 * (1 << k) * set_bits[k] for k in range(bits)]
    zone = v // (n_vocab // 4)
    top = 3 * n_vocab // 4

    def across(mask):
        return functools.reduce(lambda a, b: a + b, [steps[k] for k in range(bits) if mask >> k & 1], v)

    partner = across(1)
    far = jnp.where(odd == 1, above, below)
    last = tokens - TOK_EDGE
    targets = (partner, far)
    firsts = tuple(
        pl.multiple_of(first, TOK_EDGE) for first in ((1 - odd) * last, odd * last)
    )
    bases = tuple(
        pl.multiple_of(base, EDGE) for base in ((1 - odd) * (rows - EDGE), odd * (rows - EDGE))
    )

    def columns(core, start, count):
        return pl.ds(pl.multiple_of(core * half + start, 128), count)

    def remote(src, dst, send, recv, device):
        return pltpu.make_async_remote_copy(
            src_ref=src, dst_ref=dst, send_sem=send, recv_sem=recv,
            device_id={"vocab": device[0], "dp": device[1]}, device_id_type=MESH,
        )

    barrier = pltpu.get_barrier_semaphore()

    def greet(w, core):
        pl.semaphore_signal(
            barrier, inc=1, device_id={"vocab": w, "dp": core}, device_id_type=MESH
        )

    def at_place(quarter, second, core=None):
        here = jnp.logical_and(zone == quarter, set_bits[1] == second)
        return here if core is None else jnp.logical_and(here, p == core)

    relay = across(top + 1)
    beyond = across(top)
    via = far + jnp.where(odd == 1, 1, -1)
    far_quarter = far // (n_vocab // 4)

    for core in range(n_dp):
        greet(partner, core)
    greet(v, mate)
    stage_copies = [
        pltpu.make_async_copy(
            grad_ref.at[0, pl.ds(firsts[0], TOK_EDGE), pl.ds(core * half, plan[0][2])],
            stage.at[core], stage_sem,
        )
        for core in range(n_dp)
    ]
    for copy in stage_copies:
        copy.start()
    for k in range(1, bits):
        pl.when(set_bits[k] == 0)(functools.partial(greet, across(1 << k), p))
    awaited = n_dp + 1 + sum(set_bits[1:])
    for quarter, second in sorted({key[:2] for key in RELAYED}):
        pl.when(at_place(3 - quarter, second))(functools.partial(greet, relay, p))
        awaited += at_place(quarter, second).astype(jnp.int32)
    own_half = pl.ds(pl.multiple_of(p * half, half), half)
    own_copy = pltpu.make_async_copy(
        grad_ref.at[0, :, own_half], toks.at[pl.ds(0, tokens), :], own_sem
    )
    own_copy.start()
    own_id_copy = pltpu.make_async_copy(ids_ref, own_ids, own_id_sem)
    own_id_copy.start()
    table_copy = pltpu.make_async_copy(table_ref.at[:, own_half], table, table_sem)
    pltpu.make_async_copy(stage, stage, stage_sem).wait()
    pl.semaphore_wait(barrier, awaited)

    def source(at, core):
        k, start, count, _ = plan[at]
        return grad_ref.at[0, pl.ds(firsts[k], TOK_EDGE), pl.ds(core * half + start, count)]

    def place(at):
        k, start, count, _ = plan[at]
        return halo.at[k, p, :, pl.ds(start, count)]

    def send_chunk(at, cores=tuple(range(n_dp))):
        k, _, _, group = plan[at]
        for core in cores:
            copy = remote(
                stage.at[core] if at == 0 else source(at, core), place(at),
                halo_send, halo_recv.at[group], (targets[k], core),
            )
            around = [
                at_place(*key) for key, flows in RELAYED.items()
                if (at, core) in [flow[1:3] for flow in flows]
            ]
            if at == FAR_NARROW:
                around = [by_way(*key) for key, count in FAR_RELAYED.items() if core < count]
            if around:
                pl.when(jnp.logical_not(functools.reduce(jnp.logical_or, around)))(copy.start)
            else:
                copy.start()

    def relay_slots(first, count, send, recv):
        slots = relayed.at[pl.ds(first, count)]
        return remote(slots, slots, send, recv, (partner, p))

    def by_way(quarter, core):
        here = jnp.logical_and(far_quarter == quarter, set_bits[1] == 1)
        return jnp.logical_and(here, p == core)

    def send_ids(k):
        for core in range(n_dp):
            remote(
                ids_ref.at[:, pl.ds(firsts[k], TOK_EDGE)], halo_ids.at[k, p],
                halo_id_send, halo_id_recv, (targets[k], core),
            ).start()

    for key, flows in RELAYED.items():
        @pl.when(at_place(*key))
        def _():
            for slot, at, core in flows:
                remote(
                    source(at, core), relayed.at[slot], halo_send, relay_recv, (relay, p)
                ).start()

    send_chunk(0)
    send_chunk(1)
    mate_copy = remote(
        grad_ref.at[0, :, columns(mate, 0, half)], toks.at[pl.ds(tokens, tokens), :],
        mate_sem.at[0], mate_sem.at[1], (v, mate),
    )
    mate_copy.start()
    mate_id_copy = remote(
        ids_ref, mate_ids, mate_id_sem.at[0], mate_id_sem.at[1], (v, mate)
    )
    mate_id_copy.start()
    send_ids(0)
    table_copy.start()

    def tell(k):
        pl.semaphore_signal(
            known_sem.at[k - 1], inc=1,
            device_id={"vocab": across(1 << k), "dp": p}, device_id_type=MESH,
        )

    for k in range(1, bits):
        pl.when(set_bits[k] == 1)(functools.partial(tell, k))
        pl.semaphore_wait(known_sem.at[k - 1], 1)
        pl.when(set_bits[k] == 0)(functools.partial(tell, k))
    send_ids(1)

    for key, count in FAR_RELAYED.items():
        @pl.when(by_way(*key))
        def _():
            for core in range(count):
                remote(
                    source(FAR_NARROW, core), relayed.at[SLOTS + core], halo_send, far_recv, (via, p)
                ).start()

    for at in (2, FAR_NARROW, 3, 4, 5):
        send_chunk(at)
    for (quarter, second, core), flows in RELAYED.items():
        @pl.when(at_place(3 - quarter, second, core))
        def _():
            relay_slots(0, len(flows), relay_send, relay_recv).wait_recv()
            for slot, at, target in flows:
                remote(
                    relayed.at[slot], place(at), relay_send, halo_recv.at[plan[at][3]],
                    (beyond, target),
                ).start()

    def forward_far():
        for (quarter, core), count in FAR_RELAYED.items():
            @pl.when(at_place(quarter, 0, core))
            def _():
                relay_slots(SLOTS, count, far_send, far_recv).wait_recv()
                for target in range(count):
                    remote(
                        relayed.at[SLOTS + target], place(FAR_NARROW), far_send,
                        halo_recv.at[plan[FAR_NARROW][3]], (partner, target),
                    ).start()

    own_start = v * rows

    def local(ids):
        shifted = ids - own_start
        return jnp.where(shifted < 0, shifted + n_vocab * rows, shifted)

    def onehot(ids, base, count):
        index = lax.broadcasted_iota(jnp.int32, (count, ids.shape[1]), 0) + base
        return jnp.where(ids == index, 1.0, 0.0).astype(jnp.bfloat16)

    def add_squares(values):
        count, wide = values.shape
        lanes = jnp.sum((values * values).reshape(count // 8, 8, wide), axis=0)
        square[...] += functools.reduce(
            jnp.add, [lanes[:, i * 128:(i + 1) * 128] for i in range(wide // 128)]
        )

    square[...] = jnp.zeros_like(square)
    own_id_copy.wait()
    mate_id_copy.wait()
    own_copy.wait()
    mate_copy.wait()

    window_ids = local(jnp.concatenate([own_ids[...], mate_ids[...]], axis=1))
    for block in range(blocks):
        if block == 1:
            forward_far()
            for core in range(n_dp):
                for at in (6, 7):
                    send_chunk(at, (core,))
        picked = onehot(window_ids, block * EDGE, EDGE)

        @pl.loop(0, half // COLS)
        def _(chunk):
            here = pl.ds(pl.multiple_of(chunk * COLS, COLS), COLS)
            part = jnp.dot(picked, toks[:, here], preferred_element_type=jnp.float32)
            grad[pl.ds(block * EDGE, EDGE), here] = part
            if 0 < block < blocks - 1:
                add_squares(part)

    remote(halo_ids, halo_ids, halo_id_send, halo_id_recv, (partner, p)).wait_recv()
    picks = []
    for k in range(2):
        ids = local(jnp.concatenate([halo_ids[k, core] for core in range(n_dp)], axis=1))
        picks.append(onehot(ids, bases[k], EDGE))
    table_copy.wait()
    for group, (k, first, size) in enumerate(groups_of(plan)):
        arrived = halo.at[k, :, :, pl.ds(first, size)]
        remote(arrived, arrived, halo_send, halo_recv.at[group], (partner, p)).wait_recv()
        for start in range(first, first + size, PIECE):
            count = min(PIECE, first + size - start)
            here = pl.ds(start, count)
            part = jnp.dot(
                picks[k], halo[k, :, :, here].reshape(n_dp * TOK_EDGE, count),
                preferred_element_type=jnp.float32,
            )
            total = grad[pl.ds(bases[k], EDGE), here] + part
            grad[pl.ds(bases[k], EDGE), here] = total
            add_squares(total)

    sums[me] = jnp.sum(square[...], axis=0, keepdims=True)
    for w in range(n_vocab):
        for core in range(n_dp):
            copy = remote(sums.at[me], sums.at[me], sum_send, sum_recv, (w, core))
            pl.when(me != w * n_dp + core)(copy.start)
    remote(halo, halo, halo_send, halo_recv.at[0], (partner, p)).wait_send()
    remote(halo_ids, halo_ids, halo_id_send, halo_id_recv, (partner, p)).wait_send()
    for (quarter, second, core), flows in RELAYED.items():
        pl.when(at_place(3 - quarter, second, core))(
            relay_slots(0, len(flows), relay_send, relay_recv).wait_send
        )
    for (quarter, core), count in FAR_RELAYED.items():
        pl.when(at_place(quarter, 0, core))(
            relay_slots(SLOTS, count, far_send, far_recv).wait_send
        )
    others = sums.at[pl.ds(0, n - 1)]
    all_sums = remote(others, others, sum_send, sum_recv, (partner, p))
    all_sums.wait_recv()

    total = jnp.sum(jnp.sum(sums[...], axis=0), axis=1, keepdims=True)
    rms = jnp.sqrt(total / (n_vocab * rows * width))
    clip_scale = 1.0 / jnp.maximum(1.0, rms / norm_limit)
    norm_ref[0:1, :] = jnp.broadcast_to(step_rate * clip_scale, (1, 128))
    norm_ref[1:2, :] = jnp.broadcast_to(rms, (1, 128))
    all_sums.wait_send()


def update(grad, table, norm_ref, out_ref, rms_ref, outbuf, rms_held, out_sem, rms_sem):
    rms_held[0] = norm_ref[1, 0]
    rms_copy = pltpu.make_async_copy(rms_held, rms_ref, rms_sem)
    rms_copy.start()
    rate = norm_ref[0:1, 0:1]
    for block in range(grad.shape[0] // STORE_ROWS):
        here = pl.ds(block * STORE_ROWS, STORE_ROWS)
        for start in range(0, grad.shape[1], STORE_COLS):
            at = (here, pl.ds(start, STORE_COLS))
            moved = table[at].astype(jnp.float32) - rate * grad[at]
            outbuf[at] = moved.astype(jnp.bfloat16)
        pltpu.make_async_copy(outbuf.at[here, :], out_ref.at[here, :], out_sem).start()
    pltpu.make_async_copy(outbuf, out_ref, out_sem).wait()
    rms_copy.wait()


def solution(mesh):
    n_vocab, n_dp = mesh.shape["vocab"], mesh.shape["dp"]
    n = n_vocab * n_dp
    bits = n_vocab.bit_length() - 1

    def body(embed_table, token_ids, grad_rows):
        rows, width = embed_table.shape
        tokens = token_ids.shape[1]
        half = width // n_dp
        plan = chunk_plan(half)
        in_vmem = pl.BlockSpec(memory_space=pltpu.VMEM)
        in_hbm = pl.BlockSpec(memory_space=pltpu.HBM)
        grad, table, norm = pl.pallas_call(
            functools.partial(kernel, (n_vocab, n_dp)),
            name="clipped_update",
            out_shape=(
                jax.ShapeDtypeStruct((rows, half), jnp.float32),
                jax.ShapeDtypeStruct((rows, half), jnp.bfloat16),
                jax.ShapeDtypeStruct((8, 128), jnp.float32),
            ),
            in_specs=[in_hbm, in_hbm, in_hbm],
            out_specs=(in_vmem, in_vmem, in_vmem),
            scratch_shapes=[
                pltpu.VMEM((n_dp * tokens, half), jnp.bfloat16),
                pltpu.VMEM((2, n_dp, TOK_EDGE, half), jnp.bfloat16),
                pltpu.VMEM((n_dp, TOK_EDGE, plan[0][2]), jnp.bfloat16),
                pltpu.VMEM((SLOTS + max(FAR_RELAYED.values()), TOK_EDGE, 128), jnp.bfloat16),
                pltpu.VMEM((1, tokens), jnp.int32),
                pltpu.VMEM((1, tokens), jnp.int32),
                pltpu.VMEM((2, n_dp, 1, TOK_EDGE), jnp.int32),
                pltpu.VMEM((8, 128), jnp.float32),
                pltpu.VMEM((n, 1, 128), jnp.float32),
                pltpu.SemaphoreType.DMA,
                pltpu.SemaphoreType.DMA,
                pltpu.SemaphoreType.DMA,
                pltpu.SemaphoreType.DMA,
                pltpu.SemaphoreType.DMA((2,)),
                pltpu.SemaphoreType.DMA((2,)),
                pltpu.SemaphoreType.DMA,
                pltpu.SemaphoreType.DMA((len(groups_of(plan)),)),
                pltpu.SemaphoreType.DMA,
                pltpu.SemaphoreType.DMA,
                pltpu.SemaphoreType.DMA,
                pltpu.SemaphoreType.DMA,
                pltpu.SemaphoreType.DMA,
                pltpu.SemaphoreType.DMA,
                pltpu.SemaphoreType.DMA,
                pltpu.SemaphoreType.DMA,
                pltpu.SemaphoreType.REGULAR((max(bits - 1, 1),)),
            ],
            compiler_params=pltpu.CompilerParams(
                collective_id=0, has_side_effects=True, vmem_limit_bytes=40 * 1024 * 1024
            ),
        )(*(pltpu.with_memory_space_constraint(x, pltpu.HBM) for x in (embed_table, token_ids, grad_rows)))
        updated, grad_rms = pl.pallas_call(
            update,
            name="clipped_step",
            out_shape=(
                jax.ShapeDtypeStruct((rows, half), jnp.bfloat16),
                jax.ShapeDtypeStruct((1,), jnp.float32),
            ),
            in_specs=[in_vmem, in_vmem, in_vmem],
            out_specs=(in_hbm, in_hbm),
            scratch_shapes=[
                pltpu.VMEM((rows, half), jnp.bfloat16),
                pltpu.SMEM((1,), jnp.float32),
                pltpu.SemaphoreType.DMA,
                pltpu.SemaphoreType.DMA,
            ],
            compiler_params=pltpu.CompilerParams(vmem_limit_bytes=24 * 1024 * 1024),
        )(grad, table, norm)
        return updated, grad_rms

    in_specs = (P("vocab", None), P("dp", "vocab"), P("dp", "vocab", None))
    out_specs = (P("vocab", "dp"), P())
    return jax.shard_map(body, mesh=mesh, in_specs=in_specs, out_specs=out_specs, check_vma=False)
```

```python
import functools

import jax
import jax.numpy as jnp
from jax import lax
from jax.experimental import pallas as pl
from jax.experimental.pallas import tpu as pltpu
from jax.sharding import PartitionSpec as P

MESH = pl.DeviceIdType.MESH
TOK_EDGE = 128
EDGE = 256
COLS = 512
STORE_ROWS = 16
STORE_COLS = 256

step_rate = 0.5
norm_limit = 1.0


PIECE = 512

RELAYED = {
    (2, 0, 0): ((0, 3, 0),),
    (2, 1, 0): ((0, 3, 0),),
    (3, 0, 0): ((0, 3, 0), (1, 3, 1)),
    (3, 0, 1): ((0, 3, 0), (1, 3, 1)),
    (3, 1, 0): ((0, 3, 0), (1, 3, 1)),
    (3, 1, 1): ((0, 3, 0), (1, 3, 1)),
}
SLOTS = 2
FAR_NARROW = 8
FAR_RELAYED = {(0, 0): 1, (1, 0): 1, (1, 1): 1, (2, 0): 1, (3, 0): 1}


def chunk_plan(half):
    quarter = half // 4
    narrow = 128
    return (
        (0, 0, quarter, 0),
        (0, quarter, 2 * narrow, 0),
        (1, 0, half - narrow, 1),
        (0, quarter + 2 * narrow, narrow, 2),
        (0, quarter + 3 * narrow, narrow, 3),
        (0, 2 * quarter, 2 * quarter - 2 * narrow, 4),
        (0, half - 2 * narrow, narrow, 5),
        (0, half - narrow, narrow, 7),
        (1, half - narrow, narrow, 6),
    )


def groups_of(plan):
    groups = {}
    for k, start, count, group in plan:
        first = groups.get(group, (k, start, 0))
        groups[group] = (k, first[1], first[2] + count)
    return [groups[group] for group in sorted(groups)]


def kernel(sizes, table_ref, ids_ref, grad_ref, grad, table, norm_ref,
           toks, halo, stage, relayed, own_ids, mate_ids, halo_ids, square, sums,
           own_sem, own_id_sem, table_sem, stage_sem, mate_sem, mate_id_sem,
           halo_send, halo_recv, halo_id_send, halo_id_recv, sum_send, sum_recv,
           relay_send, relay_recv, far_send, far_recv, known_sem):
    n_vocab, n_dp = sizes
    rows, width = table_ref.shape
    tokens = ids_ref.shape[1]
    half = width // n_dp
    n = n_vocab * n_dp
    blocks = rows // EDGE
    bits = n_vocab.bit_length() - 1
    plan = chunk_plan(half)
    v = lax.axis_index("vocab")
    p = lax.axis_index("dp")
    me = v * n_dp + p
    mate = 1 - p
    odd = lax.rem(v, 2)
    below = lax.rem(v + n_vocab - 1, n_vocab)
    above = lax.rem(v + 1, n_vocab)
    set_bits = [lax.rem(v // (1 << k), 2) for k in range(bits)]
    steps = [(1 << k) - 2 * (1 << k) * set_bits[k] for k in range(bits)]
    zone = v // (n_vocab // 4)
    top = 3 * n_vocab // 4

    def across(mask):
        return functools.reduce(lambda a, b: a + b, [steps[k] for k in range(bits) if mask >> k & 1], v)

    partner = across(1)
    far = jnp.where(odd == 1, above, below)
    last = tokens - TOK_EDGE
    targets = (partner, far)
    firsts = tuple(
        pl.multiple_of(first, TOK_EDGE) for first in ((1 - odd) * last, odd * last)
    )
    bases = tuple(
        pl.multiple_of(base, EDGE) for base in ((1 - odd) * (rows - EDGE), odd * (rows - EDGE))
    )

    def columns(core, start, count):
        return pl.ds(pl.multiple_of(core * half + start, 128), count)

    def remote(src, dst, send, recv, device):
        return pltpu.make_async_remote_copy(
            src_ref=src, dst_ref=dst, send_sem=send, recv_sem=recv,
            device_id={"vocab": device[0], "dp": device[1]}, device_id_type=MESH,
        )

    barrier = pltpu.get_barrier_semaphore()

    def greet(w, core):
        pl.semaphore_signal(
            barrier, inc=1, device_id={"vocab": w, "dp": core}, device_id_type=MESH
        )

    def at_place(quarter, second, core=None):
        here = jnp.logical_and(zone == quarter, set_bits[1] == second)
        return here if core is None else jnp.logical_and(here, p == core)

    relay = across(top + 1)
    beyond = across(top)
    via = far + jnp.where(odd == 1, 1, -1)
    far_quarter = far // (n_vocab // 4)

    for core in range(n_dp):
        greet(partner, core)
    greet(v, mate)
    stage_copies = [
        pltpu.make_async_copy(
            grad_ref.at[0, pl.ds(firsts[0], TOK_EDGE), pl.ds(core * half, plan[0][2])],
            stage.at[core], stage_sem,
        )
        for core in range(n_dp)
    ]
    for copy in stage_copies:
        copy.start()
    for k in range(1, bits):
        pl.when(set_bits[k] == 0)(functools.partial(greet, across(1 << k), p))
    awaited = n_dp + 1 + sum(set_bits[1:])
    for quarter, second in sorted({key[:2] for key in RELAYED}):
        pl.when(at_place(3 - quarter, second))(functools.partial(greet, relay, p))
        awaited += at_place(quarter, second).astype(jnp.int32)
    own_half = pl.ds(pl.multiple_of(p * half, half), half)
    own_copy = pltpu.make_async_copy(
        grad_ref.at[0, :, own_half], toks.at[pl.ds(0, tokens), :], own_sem
    )
    own_copy.start()
    own_id_copy = pltpu.make_async_copy(ids_ref, own_ids, own_id_sem)
    own_id_copy.start()
    table_copy = pltpu.make_async_copy(table_ref.at[:, own_half], table, table_sem)
    pltpu.make_async_copy(stage, stage, stage_sem).wait()
    pl.semaphore_wait(barrier, awaited)

    def source(at, core):
        k, start, count, _ = plan[at]
        return grad_ref.at[0, pl.ds(firsts[k], TOK_EDGE), pl.ds(core * half + start, count)]

    def place(at):
        k, start, count, _ = plan[at]
        return halo.at[k, p, :, pl.ds(start, count)]

    def send_chunk(at, cores=tuple(range(n_dp))):
        k, _, _, group = plan[at]
        for core in cores:
            copy = remote(
                stage.at[core] if at == 0 else source(at, core), place(at),
                halo_send, halo_recv.at[group], (targets[k], core),
            )
            around = [
                at_place(*key) for key, flows in RELAYED.items()
                if (at, core) in [flow[1:3] for flow in flows]
            ]
            if at == FAR_NARROW:
                around = [by_way(*key) for key, count in FAR_RELAYED.items() if core < count]
            if around:
                pl.when(jnp.logical_not(functools.reduce(jnp.logical_or, around)))(copy.start)
            else:
                copy.start()

    def relay_slots(first, count, send, recv):
        slots = relayed.at[pl.ds(first, count)]
        return remote(slots, slots, send, recv, (partner, p))

    def by_way(quarter, core):
        here = jnp.logical_and(far_quarter == quarter, set_bits[1] == 1)
        return jnp.logical_and(here, p == core)

    def send_ids(k):
        for core in range(n_dp):
            remote(
                ids_ref.at[:, pl.ds(firsts[k], TOK_EDGE)], halo_ids.at[k, p],
                halo_id_send, halo_id_recv, (targets[k], core),
            ).start()

    for key, flows in RELAYED.items():
        @pl.when(at_place(*key))
        def _():
            for slot, at, core in flows:
                remote(
                    source(at, core), relayed.at[slot], halo_send, relay_recv, (relay, p)
                ).start()

    send_chunk(0)
    send_chunk(1)
    mate_copy = remote(
        grad_ref.at[0, :, columns(mate, 0, half)], toks.at[pl.ds(tokens, tokens), :],
        mate_sem.at[0], mate_sem.at[1], (v, mate),
    )
    mate_copy.start()
    mate_id_copy = remote(
        ids_ref, mate_ids, mate_id_sem.at[0], mate_id_sem.at[1], (v, mate)
    )
    mate_id_copy.start()
    send_ids(0)
    table_copy.start()

    def tell(k):
        pl.semaphore_signal(
            known_sem.at[k - 1], inc=1,
            device_id={"vocab": across(1 << k), "dp": p}, device_id_type=MESH,
        )

    for k in range(1, bits):
        pl.when(set_bits[k] == 1)(functools.partial(tell, k))
        pl.semaphore_wait(known_sem.at[k - 1], 1)
        pl.when(set_bits[k] == 0)(functools.partial(tell, k))
    send_ids(1)

    for key, count in FAR_RELAYED.items():
        @pl.when(by_way(*key))
        def _():
            for core in range(count):
                remote(
                    source(FAR_NARROW, core), relayed.at[SLOTS + core], halo_send, far_recv, (via, p)
                ).start()

    for at in (2, FAR_NARROW, 3, 4, 5):
        send_chunk(at)
    for (quarter, second, core), flows in RELAYED.items():
        @pl.when(at_place(3 - quarter, second, core))
        def _():
            relay_slots(0, len(flows), relay_send, relay_recv).wait_recv()
            for slot, at, target in flows:
                remote(
                    relayed.at[slot], place(at), relay_send, halo_recv.at[plan[at][3]],
                    (beyond, target),
                ).start()

    def forward_far():
        for (quarter, core), count in FAR_RELAYED.items():
            @pl.when(at_place(quarter, 0, core))
            def _():
                relay_slots(SLOTS, count, far_send, far_recv).wait_recv()
                for target in range(count):
                    remote(
                        relayed.at[SLOTS + target], place(FAR_NARROW), far_send,
                        halo_recv.at[plan[FAR_NARROW][3]], (partner, target),
                    ).start()

    own_start = v * rows

    def local(ids):
        shifted = ids - own_start
        return jnp.where(shifted < 0, shifted + n_vocab * rows, shifted)

    def onehot(ids, base, count):
        index = lax.broadcasted_iota(jnp.int32, (count, ids.shape[1]), 0) + base
        return jnp.where(ids == index, 1.0, 0.0).astype(jnp.bfloat16)

    def add_squares(values):
        count, wide = values.shape
        lanes = jnp.sum((values * values).reshape(count // 8, 8, wide), axis=0)
        square[...] += functools.reduce(
            jnp.add, [lanes[:, i * 128:(i + 1) * 128] for i in range(wide // 128)]
        )

    square[...] = jnp.zeros_like(square)
    own_id_copy.wait()
    mate_id_copy.wait()
    own_copy.wait()
    mate_copy.wait()

    window_ids = local(jnp.concatenate([own_ids[...], mate_ids[...]], axis=1))
    for block in range(blocks):
        if block == 1:
            forward_far()
            for core in range(n_dp):
                for at in (6, 7):
                    send_chunk(at, (core,))
        picked = onehot(window_ids, block * EDGE, EDGE)

        @pl.loop(0, half // COLS)
        def _(chunk):
            here = pl.ds(pl.multiple_of(chunk * COLS, COLS), COLS)
            part = jnp.dot(picked, toks[:, here], preferred_element_type=jnp.float32)
            grad[pl.ds(block * EDGE, EDGE), here] = part
            if 0 < block < blocks - 1:
                add_squares(part)

    remote(halo_ids, halo_ids, halo_id_send, halo_id_recv, (partner, p)).wait_recv()
    picks = []
    for k in range(2):
        ids = local(jnp.concatenate([halo_ids[k, core] for core in range(n_dp)], axis=1))
        picks.append(onehot(ids, bases[k], EDGE))
    table_copy.wait()
    for group, (k, first, size) in enumerate(groups_of(plan)):
        arrived = halo.at[k, :, :, pl.ds(first, size)]
        remote(arrived, arrived, halo_send, halo_recv.at[group], (partner, p)).wait_recv()
        for start in range(first, first + size, PIECE):
            count = min(PIECE, first + size - start)
            here = pl.ds(start, count)
            part = jnp.dot(
                picks[k], halo[k, :, :, here].reshape(n_dp * TOK_EDGE, count),
                preferred_element_type=jnp.float32,
            )
            total = grad[pl.ds(bases[k], EDGE), here] + part
            grad[pl.ds(bases[k], EDGE), here] = total
            add_squares(total)

    sums[me] = jnp.sum(square[...], axis=0, keepdims=True)
    for w in range(n_vocab):
        for core in range(n_dp):
            copy = remote(sums.at[me], sums.at[me], sum_send, sum_recv, (w, core))
            pl.when(me != w * n_dp + core)(copy.start)
    remote(halo, halo, halo_send, halo_recv.at[0], (partner, p)).wait_send()
    remote(halo_ids, halo_ids, halo_id_send, halo_id_recv, (partner, p)).wait_send()
    for (quarter, second, core), flows in RELAYED.items():
        pl.when(at_place(3 - quarter, second, core))(
            relay_slots(0, len(flows), relay_send, relay_recv).wait_send
        )
    for (quarter, core), count in FAR_RELAYED.items():
        pl.when(at_place(quarter, 0, core))(
            relay_slots(SLOTS, count, far_send, far_recv).wait_send
        )
    others = sums.at[pl.ds(0, n - 1)]
    all_sums = remote(others, others, sum_send, sum_recv, (partner, p))
    all_sums.wait_recv()

    total = jnp.sum(jnp.sum(sums[...], axis=0), axis=1, keepdims=True)
    rms = jnp.sqrt(total / (n_vocab * rows * width))
    norm_ref[0:1, :] = jnp.broadcast_to(step_rate / jnp.maximum(1.0, rms / norm_limit), (1, 128))
    norm_ref[1:2, :] = jnp.broadcast_to(rms, (1, 128))
    all_sums.wait_send()


def update(grad, table, norm_ref, out_ref, rms_ref, outbuf, rms_held, out_sem, rms_sem):
    rms_held[0] = norm_ref[1, 0]
    rms_copy = pltpu.make_async_copy(rms_held, rms_ref, rms_sem)
    rms_copy.start()
    rate = jnp.concatenate([norm_ref[0:1, :]] * (STORE_COLS // 128), axis=1)
    for block in range(grad.shape[0] // STORE_ROWS):
        here = pl.ds(block * STORE_ROWS, STORE_ROWS)
        for start in range(0, grad.shape[1], STORE_COLS):
            at = (here, pl.ds(start, STORE_COLS))
            moved = table[at].astype(jnp.float32) - rate * grad[at]
            outbuf[at] = moved.astype(jnp.bfloat16)
        pltpu.make_async_copy(outbuf.at[here, :], out_ref.at[here, :], out_sem).start()
    pltpu.make_async_copy(outbuf, out_ref, out_sem).wait()
    rms_copy.wait()


def solution(mesh):
    n_vocab, n_dp = mesh.shape["vocab"], mesh.shape["dp"]
    n = n_vocab * n_dp
    bits = n_vocab.bit_length() - 1

    def body(embed_table, token_ids, grad_rows):
        rows, width = embed_table.shape
        tokens = token_ids.shape[1]
        half = width // n_dp
        plan = chunk_plan(half)
        in_vmem = pl.BlockSpec(memory_space=pltpu.VMEM)
        in_hbm = pl.BlockSpec(memory_space=pltpu.HBM)
        grad, table, norm = pl.pallas_call(
            functools.partial(kernel, (n_vocab, n_dp)),
            name="clipped_update",
            out_shape=(
                jax.ShapeDtypeStruct((rows, half), jnp.float32),
                jax.ShapeDtypeStruct((rows, half), jnp.bfloat16),
                jax.ShapeDtypeStruct((8, 128), jnp.float32),
            ),
            in_specs=[in_hbm, in_hbm, in_hbm],
            out_specs=(in_vmem, in_vmem, in_vmem),
            scratch_shapes=[
                pltpu.VMEM((n_dp * tokens, half), jnp.bfloat16),
                pltpu.VMEM((2, n_dp, TOK_EDGE, half), jnp.bfloat16),
                pltpu.VMEM((n_dp, TOK_EDGE, plan[0][2]), jnp.bfloat16),
                pltpu.VMEM((SLOTS + max(FAR_RELAYED.values()), TOK_EDGE, 128), jnp.bfloat16),
                pltpu.VMEM((1, tokens), jnp.int32),
                pltpu.VMEM((1, tokens), jnp.int32),
                pltpu.VMEM((2, n_dp, 1, TOK_EDGE), jnp.int32),
                pltpu.VMEM((8, 128), jnp.float32),
                pltpu.VMEM((n, 1, 128), jnp.float32),
                pltpu.SemaphoreType.DMA,
                pltpu.SemaphoreType.DMA,
                pltpu.SemaphoreType.DMA,
                pltpu.SemaphoreType.DMA,
                pltpu.SemaphoreType.DMA((2,)),
                pltpu.SemaphoreType.DMA((2,)),
                pltpu.SemaphoreType.DMA,
                pltpu.SemaphoreType.DMA((len(groups_of(plan)),)),
                pltpu.SemaphoreType.DMA,
                pltpu.SemaphoreType.DMA,
                pltpu.SemaphoreType.DMA,
                pltpu.SemaphoreType.DMA,
                pltpu.SemaphoreType.DMA,
                pltpu.SemaphoreType.DMA,
                pltpu.SemaphoreType.DMA,
                pltpu.SemaphoreType.DMA,
                pltpu.SemaphoreType.REGULAR((max(bits - 1, 1),)),
            ],
            compiler_params=pltpu.CompilerParams(
                collective_id=0, has_side_effects=True, vmem_limit_bytes=40 * 1024 * 1024
            ),
        )(*(pltpu.with_memory_space_constraint(x, pltpu.HBM) for x in (embed_table, token_ids, grad_rows)))
        updated, grad_rms = pl.pallas_call(
            update,
            name="clipped_step",
            out_shape=(
                jax.ShapeDtypeStruct((rows, half), jnp.bfloat16),
                jax.ShapeDtypeStruct((1,), jnp.float32),
            ),
            in_specs=[in_vmem, in_vmem, in_vmem],
            out_specs=(in_hbm, in_hbm),
            scratch_shapes=[
                pltpu.VMEM((rows, half), jnp.bfloat16),
                pltpu.SMEM((1,), jnp.float32),
                pltpu.SemaphoreType.DMA,
                pltpu.SemaphoreType.DMA,
            ],
            compiler_params=pltpu.CompilerParams(vmem_limit_bytes=24 * 1024 * 1024),
        )(grad, table, norm)
        return updated, grad_rms

    in_specs = (P("vocab", None), P("dp", "vocab"), P("dp", "vocab", None))
    out_specs = (P("vocab", "dp"), P())
    return jax.shard_map(body, mesh=mesh, in_specs=in_specs, out_specs=out_specs, check_vma=False)
```

```python
import functools

import jax
import jax.numpy as jnp
from jax import lax
from jax.experimental import pallas as pl
from jax.experimental.pallas import tpu as pltpu
from jax.sharding import PartitionSpec as P

MESH = pl.DeviceIdType.MESH
TOK_EDGE = 128
EDGE = 256
COLS = 512
STORE_ROWS = 16
STORE_COLS = 256

step_rate = 0.5
norm_limit = 1.0


PIECE = 512

RELAYED = {
    (2, 0, 0): ((0, 3, 0),),
    (2, 1, 0): ((0, 3, 0),),
    (3, 0, 0): ((0, 3, 0), (1, 3, 1)),
    (3, 0, 1): ((0, 3, 0), (1, 3, 1)),
    (3, 1, 0): ((0, 3, 0), (1, 3, 1)),
    (3, 1, 1): ((0, 3, 0), (1, 3, 1)),
}
SLOTS = 2
FAR_NARROW = 8
FAR_RELAYED = {(0, 0): 1, (1, 0): 1, (1, 1): 1, (2, 0): 1, (3, 0): 1}


def chunk_plan(half):
    quarter = half // 4
    narrow = 128
    return (
        (0, 0, quarter, 0),
        (0, quarter, 2 * narrow, 0),
        (1, 0, half - narrow, 1),
        (0, quarter + 2 * narrow, narrow, 2),
        (0, quarter + 3 * narrow, narrow, 3),
        (0, 2 * quarter, 2 * quarter - 2 * narrow, 4),
        (0, half - 2 * narrow, narrow, 5),
        (0, half - narrow, narrow, 7),
        (1, half - narrow, narrow, 6),
    )


def groups_of(plan):
    groups = {}
    for k, start, count, group in plan:
        first = groups.get(group, (k, start, 0))
        groups[group] = (k, first[1], first[2] + count)
    return [groups[group] for group in sorted(groups)]


def kernel(sizes, table_ref, ids_ref, grad_ref, grad, table, norm_ref,
           toks, halo, stage, relayed, own_ids, mate_ids, halo_ids, square, sums,
           own_sem, own_id_sem, stage_sem, mate_sem, mate_id_sem,
           halo_send, halo_recv, halo_id_send, halo_id_recv, sum_send, sum_recv,
           relay_send, relay_recv, far_send, far_recv, known_sem):
    n_vocab, n_dp = sizes
    rows, width = table_ref.shape
    tokens = ids_ref.shape[1]
    half = width // n_dp
    n = n_vocab * n_dp
    blocks = rows // EDGE
    bits = n_vocab.bit_length() - 1
    plan = chunk_plan(half)
    v = lax.axis_index("vocab")
    p = lax.axis_index("dp")
    me = v * n_dp + p
    mate = 1 - p
    odd = lax.rem(v, 2)
    below = lax.rem(v + n_vocab - 1, n_vocab)
    above = lax.rem(v + 1, n_vocab)
    set_bits = [lax.rem(v // (1 << k), 2) for k in range(bits)]
    steps = [(1 << k) - 2 * (1 << k) * set_bits[k] for k in range(bits)]
    zone = v // (n_vocab // 4)
    top = 3 * n_vocab // 4

    def across(mask):
        return functools.reduce(lambda a, b: a + b, [steps[k] for k in range(bits) if mask >> k & 1], v)

    partner = across(1)
    far = jnp.where(odd == 1, above, below)
    last = tokens - TOK_EDGE
    targets = (partner, far)
    firsts = tuple(
        pl.multiple_of(first, TOK_EDGE) for first in ((1 - odd) * last, odd * last)
    )
    bases = tuple(
        pl.multiple_of(base, EDGE) for base in ((1 - odd) * (rows - EDGE), odd * (rows - EDGE))
    )

    def columns(core, start, count):
        return pl.ds(pl.multiple_of(core * half + start, 128), count)

    def remote(src, dst, send, recv, device):
        return pltpu.make_async_remote_copy(
            src_ref=src, dst_ref=dst, send_sem=send, recv_sem=recv,
            device_id={"vocab": device[0], "dp": device[1]}, device_id_type=MESH,
        )

    barrier = pltpu.get_barrier_semaphore()

    def greet(w, core):
        pl.semaphore_signal(
            barrier, inc=1, device_id={"vocab": w, "dp": core}, device_id_type=MESH
        )

    def at_place(quarter, second, core=None):
        here = jnp.logical_and(zone == quarter, set_bits[1] == second)
        return here if core is None else jnp.logical_and(here, p == core)

    relay = across(top + 1)
    beyond = across(top)
    via = far + jnp.where(odd == 1, 1, -1)
    far_quarter = far // (n_vocab // 4)

    for core in range(n_dp):
        greet(partner, core)
    greet(v, mate)
    stage_copies = [
        pltpu.make_async_copy(
            grad_ref.at[0, pl.ds(firsts[0], TOK_EDGE), pl.ds(core * half, plan[0][2])],
            stage.at[core], stage_sem,
        )
        for core in range(n_dp)
    ]
    for copy in stage_copies:
        copy.start()
    for k in range(1, bits):
        pl.when(set_bits[k] == 0)(functools.partial(greet, across(1 << k), p))
    awaited = n_dp + 1 + sum(set_bits[1:])
    for quarter, second in sorted({key[:2] for key in RELAYED}):
        pl.when(at_place(3 - quarter, second))(functools.partial(greet, relay, p))
        awaited += at_place(quarter, second).astype(jnp.int32)
    own_half = pl.ds(pl.multiple_of(p * half, half), half)
    own_copy = pltpu.make_async_copy(
        grad_ref.at[0, :, own_half], toks.at[pl.ds(0, tokens), :], own_sem
    )
    own_copy.start()
    own_id_copy = pltpu.make_async_copy(ids_ref, own_ids, own_id_sem)
    own_id_copy.start()
    table_copy = pltpu.make_async_copy(table_ref.at[:, own_half], table, stage_sem)
    pltpu.make_async_copy(stage, stage, stage_sem).wait()
    pl.semaphore_wait(barrier, awaited)

    def source(at, core):
        k, start, count, _ = plan[at]
        return grad_ref.at[0, pl.ds(firsts[k], TOK_EDGE), pl.ds(core * half + start, count)]

    def place(at):
        k, start, count, _ = plan[at]
        return halo.at[k, p, :, pl.ds(start, count)]

    def send_chunk(at, cores=tuple(range(n_dp))):
        k, _, _, group = plan[at]
        for core in cores:
            copy = remote(
                stage.at[core] if at == 0 else source(at, core), place(at),
                halo_send, halo_recv.at[group], (targets[k], core),
            )
            around = [
                at_place(*key) for key, flows in RELAYED.items()
                if (at, core) in [flow[1:3] for flow in flows]
            ]
            if at == FAR_NARROW:
                around = [by_way(*key) for key, count in FAR_RELAYED.items() if core < count]
            if around:
                pl.when(jnp.logical_not(functools.reduce(jnp.logical_or, around)))(copy.start)
            else:
                copy.start()

    def relay_slots(first, count, send, recv):
        slots = relayed.at[pl.ds(first, count)]
        return remote(slots, slots, send, recv, (partner, p))

    def by_way(quarter, core):
        here = jnp.logical_and(far_quarter == quarter, set_bits[1] == 1)
        return jnp.logical_and(here, p == core)

    def send_ids(k):
        for core in range(n_dp):
            remote(
                ids_ref.at[:, pl.ds(firsts[k], TOK_EDGE)], halo_ids.at[k, p],
                halo_id_send, halo_id_recv, (targets[k], core),
            ).start()

    for key, flows in RELAYED.items():
        @pl.when(at_place(*key))
        def _():
            for slot, at, core in flows:
                remote(
                    source(at, core), relayed.at[slot], halo_send, relay_recv, (relay, p)
                ).start()

    send_chunk(0)
    send_chunk(1)
    mate_copy = remote(
        grad_ref.at[0, :, columns(mate, 0, half)], toks.at[pl.ds(tokens, tokens), :],
        mate_sem.at[0], mate_sem.at[1], (v, mate),
    )
    mate_copy.start()
    mate_id_copy = remote(
        ids_ref, mate_ids, mate_id_sem.at[0], mate_id_sem.at[1], (v, mate)
    )
    mate_id_copy.start()
    send_ids(0)
    table_copy.start()

    def tell(k):
        pl.semaphore_signal(
            known_sem.at[k - 1], inc=1,
            device_id={"vocab": across(1 << k), "dp": p}, device_id_type=MESH,
        )

    for k in range(1, bits):
        pl.when(set_bits[k] == 1)(functools.partial(tell, k))
        pl.semaphore_wait(known_sem.at[k - 1], 1)
        pl.when(set_bits[k] == 0)(functools.partial(tell, k))
    send_ids(1)

    for key, count in FAR_RELAYED.items():
        @pl.when(by_way(*key))
        def _():
            for core in range(count):
                remote(
                    source(FAR_NARROW, core), relayed.at[SLOTS + core], halo_send, far_recv, (via, p)
                ).start()

    for at in (2, FAR_NARROW, 3, 4, 5):
        send_chunk(at)
    for (quarter, second, core), flows in RELAYED.items():
        @pl.when(at_place(3 - quarter, second, core))
        def _():
            relay_slots(0, len(flows), relay_send, relay_recv).wait_recv()
            for slot, at, target in flows:
                remote(
                    relayed.at[slot], place(at), relay_send, halo_recv.at[plan[at][3]],
                    (beyond, target),
                ).start()

    def forward_far():
        for (quarter, core), count in FAR_RELAYED.items():
            @pl.when(at_place(quarter, 0, core))
            def _():
                relay_slots(SLOTS, count, far_send, far_recv).wait_recv()
                for target in range(count):
                    remote(
                        relayed.at[SLOTS + target], place(FAR_NARROW), far_send,
                        halo_recv.at[plan[FAR_NARROW][3]], (partner, target),
                    ).start()

    own_start = v * rows

    def local(ids):
        shifted = ids - own_start
        return jnp.where(shifted < 0, shifted + n_vocab * rows, shifted)

    def onehot(ids, base, count):
        index = lax.broadcasted_iota(jnp.int32, (count, ids.shape[1]), 0) + base
        return jnp.where(ids == index, 1.0, 0.0).astype(jnp.bfloat16)

    def add_squares(values):
        count, wide = values.shape
        lanes = jnp.sum((values * values).reshape(count // 8, 8, wide), axis=0)
        square[...] += functools.reduce(
            jnp.add, [lanes[:, i * 128:(i + 1) * 128] for i in range(wide // 128)]
        )

    square[...] = jnp.zeros_like(square)
    own_id_copy.wait()
    mate_id_copy.wait()
    own_copy.wait()
    mate_copy.wait()

    window_ids = local(jnp.concatenate([own_ids[...], mate_ids[...]], axis=1))
    for block in range(blocks):
        if block == 1:
            forward_far()
            for core in range(n_dp):
                for at in (6, 7):
                    send_chunk(at, (core,))
        picked = onehot(window_ids, block * EDGE, EDGE)

        @pl.loop(0, half // COLS)
        def _(chunk):
            here = pl.ds(pl.multiple_of(chunk * COLS, COLS), COLS)
            part = jnp.dot(picked, toks[:, here], preferred_element_type=jnp.float32)
            grad[pl.ds(block * EDGE, EDGE), here] = part
            if 0 < block < blocks - 1:
                add_squares(part)

    remote(halo_ids, halo_ids, halo_id_send, halo_id_recv, (partner, p)).wait_recv()
    picks = []
    for k in range(2):
        ids = local(jnp.concatenate([halo_ids[k, core] for core in range(n_dp)], axis=1))
        picks.append(onehot(ids, bases[k], EDGE))
    table_copy.wait()
    for group, (k, first, size) in enumerate(groups_of(plan)):
        arrived = halo.at[k, :, :, pl.ds(first, size)]
        remote(arrived, arrived, halo_send, halo_recv.at[group], (partner, p)).wait_recv()
        for start in range(first, first + size, PIECE):
            count = min(PIECE, first + size - start)
            here = pl.ds(start, count)
            part = jnp.dot(
                picks[k], halo[k, :, :, here].reshape(n_dp * TOK_EDGE, count),
                preferred_element_type=jnp.float32,
            )
            total = grad[pl.ds(bases[k], EDGE), here] + part
            grad[pl.ds(bases[k], EDGE), here] = total
            add_squares(total)

    sums[me] = jnp.sum(square[...], axis=0, keepdims=True)
    for w in range(n_vocab):
        for core in range(n_dp):
            copy = remote(sums.at[me], sums.at[me], sum_send, sum_recv, (w, core))
            pl.when(me != w * n_dp + core)(copy.start)
    remote(halo, halo, halo_send, halo_recv.at[0], (partner, p)).wait_send()
    remote(halo_ids, halo_ids, halo_id_send, halo_id_recv, (partner, p)).wait_send()
    for (quarter, second, core), flows in RELAYED.items():
        pl.when(at_place(3 - quarter, second, core))(
            relay_slots(0, len(flows), relay_send, relay_recv).wait_send
        )
    for (quarter, core), count in FAR_RELAYED.items():
        pl.when(at_place(quarter, 0, core))(
            relay_slots(SLOTS, count, far_send, far_recv).wait_send
        )
    others = sums.at[pl.ds(0, n - 1)]
    all_sums = remote(others, others, sum_send, sum_recv, (partner, p))
    all_sums.wait_recv()

    total = jnp.sum(jnp.sum(sums[...], axis=0), axis=1, keepdims=True)
    rms = jnp.sqrt(total / (n_vocab * rows * width))
    norm_ref[0:1, :] = jnp.broadcast_to(step_rate / jnp.maximum(1.0, rms / norm_limit), (1, 128))
    norm_ref[1:2, :] = jnp.broadcast_to(rms, (1, 128))
    all_sums.wait_send()


def update(grad, table, norm_ref, out_ref, rms_ref, outbuf, rms_held, out_sem, rms_sem):
    rate = jnp.concatenate([norm_ref[0:1, :]] * (STORE_COLS // 128), axis=1)
    for block in range(grad.shape[0] // STORE_ROWS):
        here = pl.ds(block * STORE_ROWS, STORE_ROWS)
        for start in range(0, grad.shape[1], STORE_COLS):
            at = (here, pl.ds(start, STORE_COLS))
            moved = table[at].astype(jnp.float32) - rate * grad[at]
            outbuf[at] = moved.astype(jnp.bfloat16)
        pltpu.make_async_copy(outbuf.at[here, :], out_ref.at[here, :], out_sem).start()
    rms_held[0] = norm_ref[1, 0]
    rms_copy = pltpu.make_async_copy(rms_held, rms_ref, rms_sem)
    rms_copy.start()
    pltpu.make_async_copy(outbuf, out_ref, out_sem).wait()
    rms_copy.wait()


def solution(mesh):
    n_vocab, n_dp = mesh.shape["vocab"], mesh.shape["dp"]
    n = n_vocab * n_dp
    bits = n_vocab.bit_length() - 1

    def body(embed_table, token_ids, grad_rows):
        rows, width = embed_table.shape
        tokens = token_ids.shape[1]
        half = width // n_dp
        plan = chunk_plan(half)
        in_vmem = pl.BlockSpec(memory_space=pltpu.VMEM)
        in_hbm = pl.BlockSpec(memory_space=pltpu.HBM)
        grad, table, norm = pl.pallas_call(
            functools.partial(kernel, (n_vocab, n_dp)),
            name="clipped_update",
            out_shape=(
                jax.ShapeDtypeStruct((rows, half), jnp.float32),
                jax.ShapeDtypeStruct((rows, half), jnp.bfloat16),
                jax.ShapeDtypeStruct((8, 128), jnp.float32),
            ),
            in_specs=[in_hbm, in_hbm, in_hbm],
            out_specs=(in_vmem, in_vmem, in_vmem),
            scratch_shapes=[
                pltpu.VMEM((n_dp * tokens, half), jnp.bfloat16),
                pltpu.VMEM((2, n_dp, TOK_EDGE, half), jnp.bfloat16),
                pltpu.VMEM((n_dp, TOK_EDGE, plan[0][2]), jnp.bfloat16),
                pltpu.VMEM((SLOTS + max(FAR_RELAYED.values()), TOK_EDGE, 128), jnp.bfloat16),
                pltpu.VMEM((1, tokens), jnp.int32),
                pltpu.VMEM((1, tokens), jnp.int32),
                pltpu.VMEM((2, n_dp, 1, TOK_EDGE), jnp.int32),
                pltpu.VMEM((8, 128), jnp.float32),
                pltpu.VMEM((n, 1, 128), jnp.float32),
                pltpu.SemaphoreType.DMA,
                pltpu.SemaphoreType.DMA,
                pltpu.SemaphoreType.DMA,
                pltpu.SemaphoreType.DMA((2,)),
                pltpu.SemaphoreType.DMA((2,)),
                pltpu.SemaphoreType.DMA,
                pltpu.SemaphoreType.DMA((len(groups_of(plan)),)),
                pltpu.SemaphoreType.DMA,
                pltpu.SemaphoreType.DMA,
                pltpu.SemaphoreType.DMA,
                pltpu.SemaphoreType.DMA,
                pltpu.SemaphoreType.DMA,
                pltpu.SemaphoreType.DMA,
                pltpu.SemaphoreType.DMA,
                pltpu.SemaphoreType.DMA,
                pltpu.SemaphoreType.REGULAR((max(bits - 1, 1),)),
            ],
            compiler_params=pltpu.CompilerParams(
                collective_id=0, has_side_effects=True, vmem_limit_bytes=40 * 1024 * 1024
            ),
        )(*(pltpu.with_memory_space_constraint(x, pltpu.HBM) for x in (embed_table, token_ids, grad_rows)))
        updated, grad_rms = pl.pallas_call(
            update,
            name="clipped_step",
            out_shape=(
                jax.ShapeDtypeStruct((rows, half), jnp.bfloat16),
                jax.ShapeDtypeStruct((1,), jnp.float32),
            ),
            in_specs=[in_vmem, in_vmem, in_vmem],
            out_specs=(in_hbm, in_hbm),
            scratch_shapes=[
                pltpu.VMEM((rows, half), jnp.bfloat16),
                pltpu.SMEM((1,), jnp.float32),
                pltpu.SemaphoreType.DMA,
                pltpu.SemaphoreType.DMA,
            ],
            compiler_params=pltpu.CompilerParams(vmem_limit_bytes=24 * 1024 * 1024),
        )(grad, table, norm)
        return updated, grad_rms

    in_specs = (P("vocab", None), P("dp", "vocab"), P("dp", "vocab", None))
    out_specs = (P("vocab", "dp"), P())
    return jax.shard_map(body, mesh=mesh, in_specs=in_specs, out_specs=out_specs, check_vma=False)
```
